32 devices in a mesh: row: 8 (over z, y), col: 4 (over x, core).
Axes of the slice: x: 2, y: 2, z: 4, core: 2. Of those that a mesh axis runs over, the one named last changes fastest.
Arguments:
- coarse_kernel: bfloat16 [1024, 1024], P('row', 'col'), may hold values from -0.04453125 to 0.04453125, as said below
- correlations: bfloat16 [128, 128, 128], P(('row', 'col')), may hold values from -0.5 to 0.5
- neighbor: int32 [128], P(('row', 'col')), may hold values from 0 to 7
- pair_weight: float32 [128, 128], P('row'), may hold values from 0.13 to 7.4, as said below
- energies: float32 [16384], P(('row', 'col')), may hold values from 0.5 to 2
- start_block: float32 [16384, 64], P(('row', 'col')), may hold values from -120 to 120
Outputs:
- residual: float32 [16384, 64], P(('row', 'col'))
- coefficients: float32 [3, 64, 64], replicated
The draws below stay inside these ranges and needn't reach their ends.
Inputs may be any that keep to these rules, and one draw needn't show every extreme that they name: coarse_kernel equals its transpose. pair_weight equals its transpose.
All inputs are finite; a program needn't handle non-finite values.
Results may differ from the reference program's by a relative error of at most 0.0085.
Values may be sent and summed in bfloat16 or wider, within the bound.
No kernel may reach another device: no remote copies, remote signals or barrier semaphores. Data moves between devices by JAX's collectives and lax.ppermute only.
A program may use at most 64 MiB of HBM per device.

```python
import math
import jax
import jax.numpy as jnp
from jax import lax

B = 128
M = 64
NC = 8
NK = 128


def draw_coarse_kernel(key, part):
    noise_key = jax.random.fold_in(key, 11)
    noise = jnp.clip(jax.random.normal(noise_key, (NC * B, NC * B), jnp.float32), -4.0, 4.0)
    return ((noise + noise.T) * (0.7071 / math.sqrt(NK * B))).astype(jnp.bfloat16)


def draw_pair_weight(key, part):
    noise_key = jax.random.fold_in(key, 23)
    noise = jnp.clip(jax.random.normal(noise_key, (NK, NK), jnp.float32), -4.0, 4.0)
    return jnp.exp(0.25 * (noise + noise.T)).astype(jnp.float32)


def draw_start_block(key, part):
    total = NK * B
    position = jnp.arange(total, dtype=jnp.float32) / float(total - 1)
    row_scale = jnp.exp(position * math.log(30.0))
    noise_key = jax.random.fold_in(key, 37)
    values = jnp.clip(jax.random.normal(noise_key, (total, M), jnp.float32), -4.0, 4.0)
    return (values * row_scale[:, None]).astype(jnp.float32)


def with_ends(drawn, stream_key, low, top_value):
    spot = [jax.random.randint(jax.random.fold_in(stream_key, axis), (), 0, length) for axis, length in enumerate(drawn.shape)]
    main_axis = drawn.shape.index(max(drawn.shape))
    neighbour = spot[:main_axis] + [(spot[main_axis] + 1) % drawn.shape[main_axis]] + spot[main_axis + 1:]
    return drawn.at[tuple(spot)].set(low).at[tuple(neighbour)].set(top_value)


def block_scale(own_key, extent, pieces, least, top_value):
    factor_of, own = 1.0, jax.random.fold_in(own_key, 6)
    for axis_at, parts in pieces:
        draws = jnp.exp(jax.random.uniform(jax.random.fold_in(own, axis_at), (parts,), jnp.float32, least / len(pieces), top_value / len(pieces)))
        factor_of = factor_of * jnp.repeat(draws, extent[axis_at] // parts).reshape([-1 if axis == axis_at else 1 for axis in range(len(extent))])
    return factor_of


def normal_values(stream_key, extent, deviation, limit, pieces=(), kind=jnp.bfloat16):
    level = block_scale(stream_key, extent, pieces, -0.22, 0.18) if pieces else 1.0
    entries = jax.random.normal(stream_key, extent, jnp.float32) * deviation * level
    return jnp.minimum(jnp.maximum(entries, -limit), limit).astype(kind)


def setup_inputs(seed: int = 0) -> dict:
    keys = jax.random.split(jax.random.key(seed), 7)
    return {
        "coarse_kernel": draw_coarse_kernel(jax.random.fold_in(keys[6], 71), 0),
        "correlations": normal_values(keys[1], (NK, B, B), B ** -0.5, 0.5, ((0, 32),)),
        "neighbor": with_ends(jax.random.randint(keys[2], (NK,), 0, NC), jax.random.fold_in(keys[2], 1), 0, NC - 1).astype(jnp.int32),
        "pair_weight": draw_pair_weight(jax.random.fold_in(keys[6], 71), 0),
        "energies": jnp.clip(jnp.exp(math.log(2.0) - 1.3862944 * jax.random.uniform(keys[4], (NK * B,), jnp.float32) ** block_scale(keys[4], (NK * B,), ((0, 32),), -0.2, 0.2)), 0.5, 2.0),
        "start_block": draw_start_block(jax.random.fold_in(keys[6], 71), 0),
    }


highest = lax.Precision.HIGHEST

def coarse_products(coarse_kernel, correlations, neighbor):
    blocks = coarse_kernel.reshape(NC, B, NC, B)[:, :, neighbor, :].astype(jnp.float32)
    mapped = jnp.einsum('cakb,kbe->cake', blocks, correlations.astype(jnp.float32), precision=highest)
    return mapped.astype(jnp.bfloat16)

def apply_kernel(mapped, correlations, neighbor, pair_weight, vectors):
    group_size = 16 if NK % 16 == 0 else NK

    def one_group(index):
        offset = index * group_size
        row_correlation = lax.dynamic_slice_in_dim(correlations, offset, group_size, 0).astype(jnp.float32)
        row_neighbor = lax.dynamic_slice_in_dim(neighbor, offset, group_size, 0)
        weights = lax.dynamic_slice_in_dim(pair_weight, offset, group_size, 0)
        chosen = mapped[row_neighbor].astype(jnp.float32)
        product = jnp.einsum('kai,kaje->kije', row_correlation, chosen, precision=highest)
        kernel_rows = (product * weights[:, None, :, None]).astype(jnp.bfloat16)
        kernel_rows = kernel_rows.reshape(group_size * B, NK * B)
        return jnp.dot(kernel_rows.astype(jnp.float32), vectors.astype(jnp.float32), preferred_element_type=jnp.float32)
    result = lax.map(one_group, jnp.arange(NK // group_size, dtype=jnp.int32))
    return result.reshape(NK * B, M)

def gram_root(block):
    count = block.shape[0]
    gram_value = jnp.dot(block.T, block, precision=highest) / count
    lower = jnp.linalg.cholesky(gram_value)
    solved = jax.scipy.linalg.solve_triangular(lower, block.T, lower=True).T
    return (lower, solved)

def reference(coarse_kernel, correlations, neighbor, pair_weight, energies, start_block):
    count = NK * B
    mapped = coarse_products(coarse_kernel, correlations, neighbor)
    lower_first, basis = gram_root(start_block)
    image = energies[:, None] * basis + apply_kernel(mapped, correlations, neighbor, pair_weight, basis.astype(jnp.bfloat16))
    alpha_first = jnp.dot(basis.T, image, precision=highest) / count
    remainder = image - jnp.dot(basis, alpha_first, precision=highest)
    lower_next, second = gram_root(remainder)
    image_next = energies[:, None] * second + apply_kernel(mapped, correlations, neighbor, pair_weight, second.astype(jnp.bfloat16))
    image_next = image_next - jnp.dot(basis, lower_next, precision=highest)
    alpha_next = jnp.dot(second.T, image_next, precision=highest) / count
    residual = image_next - jnp.dot(second, alpha_next, precision=highest)
    return (residual, jnp.stack([alpha_first, lower_next, alpha_next]))
```

```python
import functools

import jax
import jax.numpy as jnp
from jax import lax
from jax.experimental import pallas as pl
from jax.experimental.pallas import tpu as pltpu
from jax.sharding import PartitionSpec as P

highest = lax.Precision.HIGHEST
AXES = ("row", "col")
SHIFT = 1.25


def build_tile(row_correlation, row_neighbor, column_correlation, column_neighbor, coarse, weights):
    band_size = row_correlation.shape[1]
    coarse_count = coarse.shape[0] // band_size
    blocks = coarse.reshape(coarse_count, band_size, coarse_count, band_size)[
        :, :, column_neighbor, :
    ]
    mapped = jnp.einsum(
        "cakb,kbe->cake", blocks, column_correlation, preferred_element_type=jnp.float32
    ).astype(jnp.bfloat16)
    chosen = mapped[row_neighbor]
    product = jnp.einsum(
        "kai,kaje->kije", row_correlation, chosen, preferred_element_type=jnp.float32
    )
    scaled = (product * weights[:, None, :, None]).astype(jnp.bfloat16)
    return scaled.reshape(
        row_correlation.shape[0] * band_size, column_correlation.shape[0] * band_size
    )


def apply_down(kernel_tile, vectors):
    partial_value = jnp.dot(
        kernel_tile,
        lax.all_gather(vectors, "row", axis=0, tiled=True),
        preferred_element_type=jnp.float32,
    )
    return lax.psum_scatter(partial_value, "col", scatter_dimension=0, tiled=True)


def general_form(coarse_kernel, correlations, neighbor, pair_weight, energies, start_block):
    row_correlation, row_neighbor = (
        lax.all_gather(correlations, "col", axis=0, tiled=True),
        lax.all_gather(neighbor, "col", axis=0, tiled=True),
    )
    column_correlation, column_neighbor = (
        lax.all_gather(correlations, "row", axis=0, tiled=True),
        lax.all_gather(neighbor, "row", axis=0, tiled=True),
    )
    coarse_strip = lax.all_gather(coarse_kernel, "row", axis=0, tiled=True)
    coarse = lax.all_gather(coarse_strip, "col", axis=1, tiled=True)
    row_count = lax.axis_size("row")
    col_count = lax.axis_size("col")
    fine_rows = pair_weight.shape[0]
    per_device = fine_rows // col_count
    weight_grid = pair_weight.reshape(fine_rows, row_count, col_count, per_device)
    weights = lax.dynamic_index_in_dim(weight_grid, lax.axis_index("col"), 2, keepdims=False)
    weights = weights.reshape(fine_rows, row_count * per_device)
    kernel_tile = build_tile(
        row_correlation, row_neighbor, column_correlation, column_neighbor, coarse, weights
    )
    total_rows = float(start_block.shape[0] * row_count * col_count)
    first_gram = (
        lax.psum(jnp.dot(start_block.T, start_block, precision=highest), ("row", "col"))
        / total_rows
    )
    lower_first = jnp.linalg.cholesky(first_gram)
    basis = jax.scipy.linalg.solve_triangular(lower_first, start_block.T, lower=True).T
    first_term = apply_down(kernel_tile, basis.astype(jnp.bfloat16))
    image = energies[:, None] * basis + first_term
    local_projection = jnp.dot(basis.T, image, precision=highest)
    summed_projection, summed_square = lax.psum(
        (local_projection, jnp.dot(image.T, image, precision=highest)), ("row", "col")
    )
    alpha_first = summed_projection / total_rows
    remainder = image - jnp.dot(basis, alpha_first, precision=highest)
    next_gram = summed_square / total_rows - jnp.dot(alpha_first.T, alpha_first, precision=highest)
    lower_next = jnp.linalg.cholesky(next_gram)
    second = jax.scipy.linalg.solve_triangular(lower_next, remainder.T, lower=True).T
    second_term = apply_down(kernel_tile, second.astype(jnp.bfloat16))
    image_next = (
        energies[:, None] * second + second_term - jnp.dot(basis, lower_next, precision=highest)
    )
    alpha_next = (
        lax.psum(jnp.dot(second.T, image_next, precision=highest), ("row", "col")) / total_rows
    )
    residual = image_next - jnp.dot(second, alpha_next, precision=highest)
    return (residual, jnp.stack([alpha_first, lower_next, alpha_next]))


def permute(value, dims, step):
    nz, ny, nx, nc = dims
    pairs = []
    for z in range(nz):
        for y in range(ny):
            for x in range(nx):
                for c in range(nc):
                    source = ((z * ny + y) * nx + x) * nc + c
                    target = (
                        (((z + step[0]) % nz) * ny + (y + step[1]) % ny) * nx + (x + step[2]) % nx
                    ) * nc + (c + step[3]) % nc
                    pairs.append((source, target))
    return lax.ppermute(value, AXES, pairs)


def gather_everywhere(block, dims):
    nz, ny, nx, nc = dims
    order = sorted(range(1, nz), key=lambda s: min(s, nz - s))
    line = jnp.concatenate([block] + [permute(block, dims, (s, 0, 0, 0)) for s in order])
    steps = [0] + order
    pieces = [(line, (0, 0))]
    for y in range(ny):
        for x in range(nx):
            if (y, x) != (0, 0):
                pieces.append((permute(line, dims, (0, y, x, 0)), (y, x)))
    found = [(value, [(s, y, x, 0) for s in steps]) for value, (y, x) in pieces]
    for c in range(1, nc):
        for value, (y, x) in pieces:
            found.append((permute(value, dims, (0, 0, 0, c)), [(s, y, x, c) for s in steps]))
    return [f[0] for f in found], [f[1] for f in found]


def sum_everywhere(value, dims):
    nz, ny, nx, nc = dims
    for axis in (3, 2, 1, 0):
        n = dims[axis]
        if n & (n - 1) == 0:
            k = 1
            while k < n:
                pairs = []
                for z in range(nz):
                    for y in range(ny):
                        for x in range(nx):
                            for c in range(nc):
                                at = [z, y, x, c]
                                to = list(at)
                                to[axis] = at[axis] ^ k
                                pairs.append(tuple(
                                    ((p[0] * ny + p[1]) * nx + p[2]) * nc + p[3] for p in (at, to)
                                ))
                value = value + lax.ppermute(value, AXES, pairs)
                k *= 2
        else:
            total = value
            for s in range(1, n):
                step = [0, 0, 0, 0]
                step[axis] = s
                total = total + permute(value, dims, tuple(step))
            value = total
    return value


def split(value):
    high = value.astype(jnp.bfloat16)
    low = (value - high.astype(jnp.float32)).astype(jnp.bfloat16)
    return high, low


def times(value, weight, transposed):
    high, low = split(value)
    n = value.shape[0]
    both = lax.dot_general(
        jnp.concatenate([high, low]),
        weight,
        (((1,), (1 if transposed else 0,)), ((), ())),
        preferred_element_type=jnp.float32,
    )
    return both[:n] + both[n:]


def nt(a, b):
    return lax.dot_general(
        a, b, (((1,), (1,)), ((), ())), precision=highest, preferred_element_type=jnp.float32
    )


def nn(a, b):
    return lax.dot_general(
        a, b, (((1,), (0,)), ((), ())), precision=highest, preferred_element_type=jnp.float32
    )


def first_kernel(points, neighbor, start, correlation, coarse, payload, turned):
    band = correlation.shape[1]
    columns = start.shape[1]
    for p in range(points):
        st = jnp.swapaxes(start[pl.ds(p * band, band), :], 0, 1)
        turned[p] = st
        u = times(st, correlation[p], True)
        payload[pl.ds(p * columns, columns), :] = u.astype(jnp.bfloat16)
    at = points * columns
    for k in range(coarse.shape[1] // band):
        payload[pl.ds(at, coarse.shape[0]), :] = coarse[:, k * band : (k + 1) * band]
        at += coarse.shape[0]
    lane = lax.broadcasted_iota(jnp.int32, (16, band), 1)
    value = jnp.zeros((16, band), jnp.float32)
    for p in range(points):
        value = jnp.where(lane == p, neighbor[p].astype(jnp.float32), value)
    payload[pl.ds(at, 16), :] = value.astype(jnp.bfloat16)


def wrapped(value, n):
    return lax.rem(value + 2 * n, n)


def middle(geometry, u_refs, coarse_refs, block_rows, weight, nbs, correlation, acc):
    dims, steps, points, columns, band, per_row, per_col = geometry
    nz, ny, nx, nc = dims
    row, col = lax.axis_index("row"), lax.axis_index("col")
    z, y, x, c = row // ny, lax.rem(row, ny), col // nc, lax.rem(col, nc)
    coarse_count = per_row * nz * ny
    acc[...] = jnp.zeros_like(acc)
    for index, ref in enumerate(u_refs):
        lines = steps[index]
        _, dy, dx, dc = lines[0]
        line_steps = [s[0] for s in lines]

        def body(at, carry, ref=ref, index=index, dy=dy, dx=dx, dc=dc, line_steps=line_steps):
            line, q = at // points, lax.rem(at, points)
            dz = jnp.int32(line_steps[0])
            for k in range(1, len(line_steps)):
                dz = jnp.where(line == k, line_steps[k], dz)
            device = (
                (wrapped(z - dz, nz) * ny + wrapped(y - dy, ny)) * nx + wrapped(x - dx, nx)
            ) * nc + wrapped(c - dc, nc)
            base = pl.multiple_of(line * block_rows + q * columns, 16)
            u = ref[pl.ds(base, columns), :].astype(jnp.float32)
            j = nbs[index * len(line_steps) + line, q]
            for p in range(points):
                w = weight[col * points + p, device * points + q]
                acc[j, p] += w * u
            return carry

        lax.fori_loop(0, len(lines) * points, body, 0, unroll=2)
    images = []
    arrays = {}
    for index, lines in enumerate(steps):
        _, dy, dx, dc = lines[0]
        arrays[(dy, dx, dc)] = index
    line_steps = [s[0] for s in steps[0]]
    coarse_at = points * columns
    for p in range(points):
        own = nbs[0, p]
        image = jnp.zeros((columns, band), jnp.float32)
        owner_row = own // per_row
        owner_z, owner_y = owner_row // ny, lax.rem(owner_row, ny)
        dz, dy = wrapped(z - owner_z, nz), wrapped(y - owner_y, ny)
        line = jnp.int32(0)
        for k in range(len(line_steps)):
            line = jnp.where(dz == line_steps[k], k, line)
        for dx in range(nx):
            for dc in range(nc):
                owner_col = wrapped(x - dx, nx) * nc + wrapped(c - dc, nc)
                for half in range(per_col):
                    j = owner_col * per_col + half
                    base = pl.multiple_of(
                        line * coarse_refs[1]
                        + coarse_at
                        + (half * per_row + lax.rem(own, per_row)) * band,
                        16,
                    )
                    block = coarse_refs[0][arrays[(0, dx, dc)]][pl.ds(base, band), :]
                    for k in range(1, ny):
                        other = coarse_refs[0][arrays[(k, dx, dc)]][pl.ds(base, band), :]
                        block = jnp.where(dy == k, other, block)
                    image += times(acc[j, p], block, True)
        images.append(times(image, correlation[p], False))
    return images


def second_kernel(geometry, block_rows, count, *refs):
    n = len(geometry[1])
    gathered = refs[:n]
    (weight, correlation, turned, energy, payload, image, grams, nbs_out, acc, nbv, nbs, sem) = refs[n:]
    _, _, points, columns, band, per_row, per_col = geometry
    lines = len(geometry[1][0])
    at = points * columns + per_row * per_col * band
    for index in range(n):
        for line in range(lines):
            tile = gathered[index][pl.ds(line * block_rows + at, 16), :].astype(jnp.float32)
            nbv[pl.ds(index * lines + line, 1), :] = tile[0:1].astype(jnp.int32)
    copy = pltpu.make_async_copy(nbv, nbs, sem)
    copy.start()
    copy.wait()
    nbs_out[...] = nbv[...]
    images = middle(geometry, gathered, (gathered, block_rows), block_rows, weight, nbs, correlation, acc)
    total = jnp.zeros((2 * columns, 2 * columns), jnp.float32)
    for p in range(points):
        st = turned[p]
        value = energy[pl.ds(p, 1), :] * st + images[p]
        image[p] = value
        payload[pl.ds(p * columns, columns), :] = times(value, correlation[p], True).astype(
            jnp.bfloat16
        )
        pair = jnp.concatenate([st, value])
        total += nt(pair, pair)
    grams[...] = total * (1.0 / count)


def third_kernel(geometry, block_rows, count, *refs):
    n = len(geometry[1])
    vectors, gathered = refs[:n], refs[n : 2 * n]
    (nbs, weight, correlation, first, energy, image, gram, acc) = refs[2 * n :]
    _, _, points, columns, band, _, _ = geometry
    images = middle(
        geometry, vectors, (gathered, block_rows), points * columns, weight, nbs, correlation, acc
    )
    total = jnp.zeros((columns, columns), jnp.float32)
    for p in range(points):
        x1 = first[p]
        value = energy[pl.ds(p, 1), :] * x1 + images[p]
        image[p] = value
        total += nt(x1, value)
    gram[...] = total * (1.0 / count)


def eliminate(matrix, right):
    n = matrix.shape[0]
    rows = lax.broadcasted_iota(jnp.int32, (n, 1), 0)
    work = jnp.concatenate([matrix, right], axis=1)
    for k in range(n):
        scale = lax.rsqrt(work[k : k + 1, k : k + 1])
        pivot = work[k : k + 1, :] * scale
        column = jnp.where(rows > k, work[:, k : k + 1] * scale, 0.0)
        work = jnp.where(rows == k, pivot, work - column * pivot)
    upper = work[:, :n]
    keep = lax.broadcasted_iota(jnp.int32, (n, n), 0) <= lax.broadcasted_iota(jnp.int32, (n, n), 1)
    return jnp.where(keep, upper, 0.0), work[:, n:]


def last_kernel(points, joint, g12_ref, turned, first, second, residual, coefficients):
    m = g12_ref.shape[0]
    g00, g01 = joint[:m, :m], joint[:m, m:]
    g11, g12 = joint[m:, m:], g12_ref[...]
    eye = (
        lax.broadcasted_iota(jnp.int32, (m, m), 0) == lax.broadcasted_iota(jnp.int32, (m, m), 1)
    ).astype(jnp.float32)
    _, solved = eliminate(g00, jnp.concatenate([eye, g01], axis=1))
    inverse_first, z1 = solved[:, :m], solved[:, m:]
    schur = g11 - nn(z1.T, z1)
    upper, inverse_second = eliminate(schur, eye)
    lower = upper.T
    alpha_first = nt(z1, inverse_first)
    lower_next = nn(inverse_first, lower)
    t_s = -nn(inverse_second, nn(z1.T, inverse_first))
    t_x = inverse_second
    p_s = nn(t_s, g01) + nn(t_x, g11)
    p_x = nn(t_s, g11) + nn(t_x, g12)
    alpha_next = nt(p_s, t_s) + nt(p_x, t_x)
    on_start = -nn(nn(upper, inverse_first.T), inverse_first) - nn(alpha_next, t_s)
    on_first = t_s - nn(alpha_next, t_x)
    coefficients[0] = alpha_first + SHIFT * eye
    coefficients[1] = lower_next
    coefficients[2] = alpha_next + SHIFT * eye
    band = turned.shape[2]
    factors = jnp.concatenate([on_start, on_first, t_x], axis=1)
    for p in range(points):
        value = nn(factors, jnp.concatenate([turned[p], first[p], second[p]]))
        residual[pl.ds(p * band, band), :] = value.T


VMEM = pl.BlockSpec(memory_space=pltpu.VMEM)
SMEM = pl.BlockSpec(memory_space=pltpu.SMEM)


def shaped(shape, dtype=jnp.float32):
    return jax.ShapeDtypeStruct(shape, dtype)


def call(kernel, name, inputs, outputs, scratch=()):
    return pl.pallas_call(
        kernel,
        name=name,
        in_specs=[spec for _, spec in inputs],
        out_shape=outputs,
        out_specs=[VMEM] * len(outputs),
        scratch_shapes=list(scratch),
        compiler_params=pltpu.CompilerParams(vmem_limit_bytes=48 * 2**20),
    )(*[value for value, _ in inputs])


def on_device(coarse_kernel, correlations, neighbor, pair_weight, energies, start_block):
    rows, cols = lax.axis_size("row"), lax.axis_size("col")
    points, band, _ = correlations.shape
    columns = start_block.shape[1]
    if rows % 2 or cols % 2 or coarse_kernel.shape[0] % band or coarse_kernel.shape[1] % band:
        return general_form(
            coarse_kernel, correlations, neighbor, pair_weight, energies, start_block
        )
    dims = (rows // 2, 2, cols // 2, 2)
    per_row, per_col = coarse_kernel.shape[0] // band, coarse_kernel.shape[1] // band
    coarse_count = per_row * rows
    count = float(start_block.shape[0] * rows * cols)
    block_rows = points * columns + per_row * per_col * band + 16
    payload, turned = call(
        functools.partial(first_kernel, points),
        "first",
        [(neighbor, SMEM), (start_block, VMEM), (correlations, VMEM), (coarse_kernel, VMEM)],
        [shaped((block_rows, band), jnp.bfloat16), shaped((points, columns, band))],
    )
    gathered, steps = gather_everywhere(payload, dims)
    geometry = (dims, steps, points, columns, band, per_row, per_col)
    shifted = energies.reshape(points, band) - SHIFT
    accumulator = pltpu.VMEM((coarse_count, points, columns, band), jnp.float32)
    devices = rows * cols
    payload, first, joint, nbs = call(
        functools.partial(second_kernel, geometry, block_rows, count),
        "second",
        [(g, VMEM) for g in gathered]
        + [(pair_weight, SMEM), (correlations, VMEM), (turned, VMEM), (shifted, VMEM)],
        [
            shaped((points * columns, band), jnp.bfloat16),
            shaped((points, columns, band)),
            shaped((2 * columns, 2 * columns)),
            shaped((devices, band), jnp.int32),
        ],
        [
            accumulator,
            pltpu.VMEM((devices, band), jnp.int32),
            pltpu.SMEM((devices, band), jnp.int32),
            pltpu.SemaphoreType.DMA,
        ],
    )
    vectors, _ = gather_everywhere(payload, dims)
    second, g12 = call(
        functools.partial(third_kernel, geometry, block_rows, count),
        "third",
        [(v, VMEM) for v in vectors]
        + [(g, VMEM) for g in gathered]
        + [(nbs, SMEM), (pair_weight, SMEM), (correlations, VMEM), (first, VMEM), (shifted, VMEM)],
        [shaped((points, columns, band)), shaped((columns, columns))],
        [accumulator],
    )
    flat = jnp.concatenate([joint.reshape(-1, band), g12.reshape(-1, band)])
    flat = sum_everywhere(flat, dims)
    size = joint.size // band
    residual, coefficients = call(
        functools.partial(last_kernel, points),
        "last",
        [
            (flat[:size].reshape(joint.shape), VMEM),
            (flat[size:].reshape(g12.shape), VMEM),
            (turned, VMEM),
            (first, VMEM),
            (second, VMEM),
        ],
        [shaped(start_block.shape), shaped((3, columns, columns))],
    )
    return residual, coefficients


def solution(mesh):
    in_specs = (
        P("row", "col"),
        P(("row", "col"), None, None),
        P(("row", "col")),
        P("row", None),
        P(("row", "col")),
        P(("row", "col"), None),
    )
    out_specs = (P(("row", "col"), None), P())
    return jax.shard_map(
        on_device, mesh=mesh, in_specs=in_specs, out_specs=out_specs, check_vma=False
    )
```

```python
import functools

import jax
import jax.numpy as jnp
from jax import lax
from jax.experimental import pallas as pl
from jax.experimental.pallas import tpu as pltpu
from jax.sharding import PartitionSpec as P

highest = lax.Precision.HIGHEST
AXES = ("row", "col")
SHIFT = 1.25
FLOPS_PER_US = 5e8


def build_tile(row_correlation, row_neighbor, column_correlation, column_neighbor, coarse, weights):
    band_size = row_correlation.shape[1]
    coarse_count = coarse.shape[0] // band_size
    blocks = coarse.reshape(coarse_count, band_size, coarse_count, band_size)[
        :, :, column_neighbor, :
    ]
    mapped = jnp.einsum(
        "cakb,kbe->cake", blocks, column_correlation, preferred_element_type=jnp.float32
    ).astype(jnp.bfloat16)
    chosen = mapped[row_neighbor]
    product = jnp.einsum(
        "kai,kaje->kije", row_correlation, chosen, preferred_element_type=jnp.float32
    )
    scaled = (product * weights[:, None, :, None]).astype(jnp.bfloat16)
    return scaled.reshape(
        row_correlation.shape[0] * band_size, column_correlation.shape[0] * band_size
    )


def apply_down(kernel_tile, vectors):
    partial_value = jnp.dot(
        kernel_tile,
        lax.all_gather(vectors, "row", axis=0, tiled=True),
        preferred_element_type=jnp.float32,
    )
    return lax.psum_scatter(partial_value, "col", scatter_dimension=0, tiled=True)


def general_form(coarse_kernel, correlations, neighbor, pair_weight, energies, start_block):
    row_correlation, row_neighbor = (
        lax.all_gather(correlations, "col", axis=0, tiled=True),
        lax.all_gather(neighbor, "col", axis=0, tiled=True),
    )
    column_correlation, column_neighbor = (
        lax.all_gather(correlations, "row", axis=0, tiled=True),
        lax.all_gather(neighbor, "row", axis=0, tiled=True),
    )
    coarse_strip = lax.all_gather(coarse_kernel, "row", axis=0, tiled=True)
    coarse = lax.all_gather(coarse_strip, "col", axis=1, tiled=True)
    row_count = lax.axis_size("row")
    col_count = lax.axis_size("col")
    fine_rows = pair_weight.shape[0]
    per_device = fine_rows // col_count
    weight_grid = pair_weight.reshape(fine_rows, row_count, col_count, per_device)
    weights = lax.dynamic_index_in_dim(weight_grid, lax.axis_index("col"), 2, keepdims=False)
    weights = weights.reshape(fine_rows, row_count * per_device)
    kernel_tile = build_tile(
        row_correlation, row_neighbor, column_correlation, column_neighbor, coarse, weights
    )
    total_rows = float(start_block.shape[0] * row_count * col_count)
    first_gram = (
        lax.psum(jnp.dot(start_block.T, start_block, precision=highest), ("row", "col"))
        / total_rows
    )
    lower_first = jnp.linalg.cholesky(first_gram)
    basis = jax.scipy.linalg.solve_triangular(lower_first, start_block.T, lower=True).T
    first_term = apply_down(kernel_tile, basis.astype(jnp.bfloat16))
    image = energies[:, None] * basis + first_term
    local_projection = jnp.dot(basis.T, image, precision=highest)
    summed_projection, summed_square = lax.psum(
        (local_projection, jnp.dot(image.T, image, precision=highest)), ("row", "col")
    )
    alpha_first = summed_projection / total_rows
    remainder = image - jnp.dot(basis, alpha_first, precision=highest)
    next_gram = summed_square / total_rows - jnp.dot(alpha_first.T, alpha_first, precision=highest)
    lower_next = jnp.linalg.cholesky(next_gram)
    second = jax.scipy.linalg.solve_triangular(lower_next, remainder.T, lower=True).T
    second_term = apply_down(kernel_tile, second.astype(jnp.bfloat16))
    image_next = (
        energies[:, None] * second + second_term - jnp.dot(basis, lower_next, precision=highest)
    )
    alpha_next = (
        lax.psum(jnp.dot(second.T, image_next, precision=highest), ("row", "col")) / total_rows
    )
    residual = image_next - jnp.dot(second, alpha_next, precision=highest)
    return (residual, jnp.stack([alpha_first, lower_next, alpha_next]))


def permute(value, dims, step):
    nz, ny, nx, nc = dims
    pairs = []
    for z in range(nz):
        for y in range(ny):
            for x in range(nx):
                for c in range(nc):
                    source = ((z * ny + y) * nx + x) * nc + c
                    target = (
                        (((z + step[0]) % nz) * ny + (y + step[1]) % ny) * nx + (x + step[2]) % nx
                    ) * nc + (c + step[3]) % nc
                    pairs.append((source, target))
    return lax.ppermute(value, AXES, pairs)


def gather_everywhere(block, dims):
    nz, ny, nx, nc = dims
    order = sorted(range(1, nz), key=lambda s: min(s, nz - s))
    line = jnp.concatenate([block] + [permute(block, dims, (s, 0, 0, 0)) for s in order])
    found = {(0, 0, 0): line}
    for y in range(ny):
        for x in range(nx):
            if (y, x) != (0, 0):
                found[(y, x, 0)] = permute(line, dims, (0, y, x, 0))
    for y in range(ny):
        for x in range(nx):
            for c in range(1, nc):
                found[(y, x, c)] = permute(found[(y, x, 0)], dims, (0, 0, 0, c))
    return list(found.values()), list(found)


def sum_everywhere(value, dims):
    nz, ny, nx, nc = dims
    for axis in (3, 2, 1, 0):
        n = dims[axis]
        if n & (n - 1) == 0:
            k = 1
            while k < n:
                pairs = []
                for z in range(nz):
                    for y in range(ny):
                        for x in range(nx):
                            for c in range(nc):
                                at = [z, y, x, c]
                                to = list(at)
                                to[axis] = at[axis] ^ k
                                pairs.append(tuple(
                                    ((p[0] * ny + p[1]) * nx + p[2]) * nc + p[3] for p in (at, to)
                                ))
                value = value + lax.ppermute(value, AXES, pairs)
                k *= 2
        else:
            total = value
            for s in range(1, n):
                step = [0, 0, 0, 0]
                step[axis] = s
                total = total + permute(value, dims, tuple(step))
            value = total
    return value


def split(value):
    high = value.astype(jnp.bfloat16)
    low = (value - high.astype(jnp.float32)).astype(jnp.bfloat16)
    return high, low


def times(value, weight, transposed):
    high, low = split(value)
    n = value.shape[0]
    both = lax.dot_general(
        jnp.concatenate([high, low]),
        weight,
        (((1,), (1 if transposed else 0,)), ((), ())),
        preferred_element_type=jnp.float32,
    )
    return both[:n] + both[n:]


def nt(a, b):
    return lax.dot_general(
        a, b, (((1,), (1,)), ((), ())), precision=highest, preferred_element_type=jnp.float32
    )


def nn(a, b):
    return lax.dot_general(
        a, b, (((1,), (0,)), ((), ())), precision=highest, preferred_element_type=jnp.float32
    )


def first_kernel(points, neighbor, start, correlation, payload, turned):
    band = correlation.shape[1]
    columns = start.shape[1]
    for p in range(points):
        st = jnp.swapaxes(start[pl.ds(p * band, band), :], 0, 1)
        turned[p] = st
        u = times(st, correlation[p], True)
        payload[pl.ds(p * columns, columns), :] = u.astype(jnp.bfloat16)
    lane = lax.broadcasted_iota(jnp.int32, (16, band), 1)
    value = jnp.zeros((16, band), jnp.float32)
    for p in range(points):
        value = jnp.where(lane == p, neighbor[p].astype(jnp.float32), value)
    payload[pl.ds(points * columns, 16), :] = value.astype(jnp.bfloat16)


def wrapped(value, n):
    return lax.rem(value + 2 * n, n)


def place(geometry):
    nz, ny, nx, nc = geometry.dims
    row, col = lax.axis_index("row"), lax.axis_index("col")
    return row // ny, lax.rem(row, ny), col // nc, lax.rem(col, nc)


def line_step(geometry, line):
    step = jnp.int32(geometry.order[0])
    for k in range(1, len(geometry.order)):
        step = jnp.where(line == k, geometry.order[k], step)
    return step


def weigh_kernel(geometry, pieces, block_rows, with_neighbors, continued, *refs):
    dims, points, columns, band = geometry.dims, geometry.points, geometry.columns, geometry.band
    nz, ny, nx, nc = dims
    lines = len(geometry.order)
    n = len(pieces)
    u_refs, refs = refs[:n], refs[n:]
    weight, refs = refs[0], refs[1:]
    if continued:
        before, refs = refs[0], refs[1:]
    if with_neighbors:
        acc, nbs_out, nbv, nbs, sem = refs
        for index in range(n):
            for line in range(lines):
                at = line * block_rows + points * columns
                tile = u_refs[index][pl.ds(at, 16), :].astype(jnp.float32)
                nbv[pl.ds(index * lines + line, 1), :] = tile[0:1].astype(jnp.int32)
        copy = pltpu.make_async_copy(nbv, nbs, sem)
        copy.start()
        nbs_out[...] = nbv[...]
    else:
        nbs, acc = refs
    acc[...] = before[...] if continued else jnp.zeros_like(acc)
    if with_neighbors:
        copy.wait()
    z, y, x, c = place(geometry)
    col = lax.axis_index("col")
    for index, ref in enumerate(u_refs):
        dy, dx, dc = pieces[index]

        def body(at, carry, ref=ref, index=index, dy=dy, dx=dx, dc=dc):
            line, q = at // points, lax.rem(at, points)
            device = (
                (wrapped(z - line_step(geometry, line), nz) * ny + wrapped(y - dy, ny)) * nx
                + wrapped(x - dx, nx)
            ) * nc + wrapped(c - dc, nc)
            base = pl.multiple_of(line * block_rows + q * columns, 16)
            u = ref[pl.ds(base, columns), :].astype(jnp.float32)
            j = nbs[index * lines + line, q]
            for p in range(points):
                w = weight[col * points + p, device * points + q]
                acc[j, p] += w * u
            return carry

        lax.fori_loop(0, lines * points, body, 0, unroll=2)


def choose_blocks(geometry, pieces, coarse_refs, own, chosen):
    nz, ny, nx, nc = geometry.dims
    band, per_row, per_col = geometry.band, geometry.per_row, geometry.per_col
    z, y, x, c = place(geometry)
    index = {piece: k for k, piece in enumerate(pieces)}
    for p in range(geometry.points):
        owner_row = own[p] // per_row
        dz = wrapped(z - owner_row // ny, nz)
        dy = wrapped(y - lax.rem(owner_row, ny), ny)
        line = jnp.int32(0)
        for k in range(len(geometry.order)):
            line = jnp.where(dz == geometry.order[k], k, line)
        base = pl.multiple_of((line * per_row + lax.rem(own[p], per_row)) * band, 16)
        for dx in range(nx):
            for dc in range(nc):
                owner_col = wrapped(x - dx, nx) * nc + wrapped(c - dc, nc)
                for k in range(per_col):
                    cut = slice(k * band, (k + 1) * band)
                    block = coarse_refs[index[(0, dx, dc)]][pl.ds(base, band), cut]
                    for d in range(1, ny):
                        other = coarse_refs[index[(d, dx, dc)]][pl.ds(base, band), cut]
                        block = jnp.where(dy == d, other, block)
                    chosen[p, owner_col * per_col + k] = block


def image_of(acc, chosen, correlation, p):
    total = times(acc[0, p], chosen[p, 0], True)
    for j in range(1, acc.shape[0]):
        total += times(acc[j, p], chosen[p, j], True)
    return times(total, correlation[p], False)


def first_image_kernel(geometry, pieces, count, *refs):
    n = len(pieces)
    coarse_refs = refs[:n]
    (acc, own, correlation, turned, energy, chosen, payload, image, grams) = refs[n:]
    columns = geometry.columns
    choose_blocks(geometry, pieces, coarse_refs, own, chosen)
    total = jnp.zeros((2 * columns, 2 * columns), jnp.float32)
    for p in range(geometry.points):
        st = turned[p]
        value = energy[pl.ds(p, 1), :] * st + image_of(acc, chosen, correlation, p)
        image[p] = value
        payload[pl.ds(p * columns, columns), :] = times(value, correlation[p], True).astype(
            jnp.bfloat16
        )
        pair = jnp.concatenate([st, value])
        total += nt(pair, pair)
    grams[...] = total * (1.0 / count)


def second_image_kernel(geometry, count, acc, chosen, correlation, first, energy, image, gram):
    columns = geometry.columns
    total = jnp.zeros((columns, columns), jnp.float32)
    for p in range(geometry.points):
        x1 = first[p]
        value = energy[pl.ds(p, 1), :] * x1 + image_of(acc, chosen, correlation, p)
        image[p] = value
        total += nt(x1, value)
    gram[...] = total * (1.0 / count)


def eliminate(work, begin, end):
    rows = lax.broadcasted_iota(jnp.int32, (work.shape[0], 1), 0)
    for k in range(begin, end):
        scale = lax.rsqrt(work[k : k + 1, k : k + 1])
        pivot = work[k : k + 1, :] * scale
        column = jnp.where(rows > k, work[:, k : k + 1] * scale, 0.0)
        work = jnp.where(rows == k, pivot, work - column * pivot)
    return work


def unit(m):
    return (
        lax.broadcasted_iota(jnp.int32, (m, m), 0) == lax.broadcasted_iota(jnp.int32, (m, m), 1)
    ).astype(jnp.float32)


def eliminate_kernel_1(joint, out):
    m = joint.shape[0] // 2
    work = jnp.concatenate([joint[:m, :m], unit(m), joint[:m, m:]], axis=1)
    out[...] = eliminate(work, 0, m // 2)


def eliminate_kernel_2(joint, given, out, schur):
    m = joint.shape[0] // 2
    work = eliminate(given[...], m // 2, m)
    out[...] = work
    z1 = work[:, 2 * m :]
    schur[...] = jnp.concatenate([joint[m:, m:] - nn(z1.T, z1), unit(m)], axis=1)


def eliminate_kernel_3(given, out):
    m = given.shape[0]
    out[...] = eliminate(given[...], 0, m // 2)


def eliminate_kernel_4(joint, one, given, first_two, parts):
    m = given.shape[0]
    work = eliminate(given[...], m // 2, m)
    keep = lax.broadcasted_iota(jnp.int32, (m, m), 0) <= lax.broadcasted_iota(jnp.int32, (m, m), 1)
    upper = jnp.where(keep, work[:, :m], 0.0)
    t_x = work[:, m:]
    inverse_first, z1 = one[:, m : 2 * m], one[:, 2 * m :]
    g01, g11 = joint[:m, m:], joint[m:, m:]
    first_two[0] = nt(z1, inverse_first) + SHIFT * unit(m)
    first_two[1] = nn(inverse_first, upper.T)
    t_s = -nn(t_x, nn(z1.T, inverse_first))
    p_s = nn(t_s, g01) + nn(t_x, g11)
    parts[0] = t_s
    parts[1] = t_x
    parts[2] = nt(p_s, t_s) + nt(nn(t_s, g11), t_x)
    parts[3] = nn(nn(upper, inverse_first.T), inverse_first)


def last_kernel(points, *refs):
    n = len(refs) - 7
    (first_two, parts, turned, first, second, residual, coefficients) = refs[n:]
    g12 = refs[0][...]
    for k in range(1, n):
        g12 += refs[k][...]
    m = g12.shape[0]
    t_s, t_x = parts[0], parts[1]
    alpha_next = parts[2] + nt(nn(t_x, g12), t_x)
    on_start = -parts[3] - nn(alpha_next, t_s)
    on_first = t_s - nn(alpha_next, t_x)
    coefficients[0] = first_two[0]
    coefficients[1] = first_two[1]
    coefficients[2] = alpha_next + SHIFT * unit(m)
    band = turned.shape[2]
    factors = jnp.concatenate([on_start, on_first, t_x], axis=1)
    for p in range(points):
        value = nn(factors, jnp.concatenate([turned[p], first[p], second[p]]))
        residual[pl.ds(p * band, band), :] = value.T


VMEM = pl.BlockSpec(memory_space=pltpu.VMEM)
SMEM = pl.BlockSpec(memory_space=pltpu.SMEM)


class Geometry:
    def __init__(self, **values):
        self.__dict__.update(values)


def shaped(shape, dtype=jnp.float32):
    return jax.ShapeDtypeStruct(shape, dtype)


def call(kernel, name, inputs, outputs, scratch=(), work=0.0, aliases=None):
    return pl.pallas_call(
        kernel,
        name=name,
        in_specs=[spec for _, spec in inputs],
        out_shape=outputs,
        out_specs=[VMEM] * len(outputs),
        scratch_shapes=list(scratch),
        input_output_aliases=aliases or {},
        cost_estimate=pl.CostEstimate(
            flops=int(work * FLOPS_PER_US), bytes_accessed=0, transcendentals=0
        ),
        compiler_params=pltpu.CompilerParams(vmem_limit_bytes=48 * 2**20),
    )(*[value for value, _ in inputs])


def weigh(geometry, arrays, pieces, block_rows, weight, neighbors, before=None):
    lines = len(geometry.order)
    shape = (geometry.coarse_count, geometry.points, geometry.columns, geometry.band)
    inputs = [(a, VMEM) for a in arrays] + [(weight, SMEM)]
    if before is not None:
        inputs.append((before, VMEM))
    at = len(inputs) - 1
    outputs = [shaped(shape)]
    scratch = []
    count = lines * len(arrays)
    if neighbors is None:
        outputs.append(shaped((count, geometry.band), jnp.int32))
        scratch = [
            pltpu.VMEM((count, geometry.band), jnp.int32),
            pltpu.SMEM((count, geometry.band), jnp.int32),
            pltpu.SemaphoreType.DMA,
        ]
    else:
        inputs.append((neighbors, SMEM))
    return call(
        functools.partial(
            weigh_kernel, geometry, pieces, block_rows, neighbors is None, before is not None
        ),
        "weigh",
        inputs,
        outputs,
        scratch,
        work=1.0 * len(arrays) / 2,
        aliases={at: 0} if before is not None else None,
    )


def on_device(coarse_kernel, correlations, neighbor, pair_weight, energies, start_block):
    rows, cols = lax.axis_size("row"), lax.axis_size("col")
    points, band, _ = correlations.shape
    columns = start_block.shape[1]
    if rows % 2 or cols % 2 or coarse_kernel.shape[0] % band or coarse_kernel.shape[1] % band:
        return general_form(
            coarse_kernel, correlations, neighbor, pair_weight, energies, start_block
        )
    dims = (rows // 2, 2, cols // 2, 2)
    order = [0] + sorted(range(1, dims[0]), key=lambda s: min(s, dims[0] - s))
    per_row, per_col = coarse_kernel.shape[0] // band, coarse_kernel.shape[1] // band
    geometry = Geometry(
        dims=dims, order=order, points=points, columns=columns, band=band,
        per_row=per_row, per_col=per_col, coarse_count=per_row * rows,
    )
    count = float(start_block.shape[0] * rows * cols)
    half = points * columns
    payload, turned = call(
        functools.partial(first_kernel, points),
        "first",
        [(neighbor, SMEM), (start_block, VMEM), (correlations, VMEM)],
        [shaped((half + 16, band), jnp.bfloat16), shaped((points, columns, band))],
        work=1.0,
    )
    shifted = energies.reshape(points, band) - SHIFT

    u, pieces = gather_everywhere(payload, dims)
    coarse, _ = gather_everywhere(coarse_kernel, dims)
    early = [k for k, piece in enumerate(pieces) if piece[:2] == (0, 0)]
    late = [k for k in range(len(pieces)) if k not in early]
    groups = [early, late]

    acc, neighbors = None, []
    for group in groups:
        acc, found = weigh(
            geometry, [u[k] for k in group], [pieces[k] for k in group], half + 16, pair_weight,
            None, acc,
        )
        neighbors.append(found)
    own = neighbors[0][0, :points]
    coarse_count = geometry.coarse_count
    chosen, payload, first, joint = call(
        functools.partial(first_image_kernel, geometry, pieces, count),
        "first_image",
        [(a, VMEM) for a in coarse]
        + [(acc, VMEM), (own, SMEM), (correlations, VMEM), (turned, VMEM), (shifted, VMEM)],
        [
            shaped((points, coarse_count, band, band), jnp.bfloat16),
            shaped((half, band), jnp.bfloat16),
            shaped((points, columns, band)),
            shaped((2 * columns, 2 * columns)),
        ],
        work=3.0,
    )
    u, _ = gather_everywhere(payload, dims)
    joint = sum_everywhere(joint, dims)
    acc = None
    for group, found in zip(groups, neighbors):
        (acc,) = weigh(
            geometry, [u[k] for k in group], [pieces[k] for k in group], half, pair_weight,
            found, acc,
        )
    second, g12 = call(
        functools.partial(second_image_kernel, geometry, count),
        "second_image",
        [(acc, VMEM), (chosen, VMEM), (correlations, VMEM), (first, VMEM), (shifted, VMEM)],
        [shaped((points, columns, band)), shaped((columns, columns))],
        work=3.0,
    )
    m = columns
    (one,) = call(
        eliminate_kernel_1, "eliminate_1", [(joint, VMEM)], [shaped((m, 3 * m))], work=3.0
    )
    one, schur = call(
        eliminate_kernel_2, "eliminate_2", [(joint, VMEM), (one, VMEM)],
        [shaped((m, 3 * m)), shaped((m, 2 * m))], work=3.0,
    )
    (two,) = call(
        eliminate_kernel_3, "eliminate_3", [(schur, VMEM)], [shaped((m, 2 * m))], work=3.0
    )
    first_two, parts = call(
        eliminate_kernel_4, "eliminate_4", [(joint, VMEM), (one, VMEM), (two, VMEM)],
        [shaped((2, m, m)), shaped((4, m, m))], work=3.0,
    )
    g12 = sum_everywhere(g12, dims)
    residual, coefficients = call(
        functools.partial(last_kernel, points),
        "last",
        [(g12, VMEM), (first_two, VMEM), (parts, VMEM), (turned, VMEM), (first, VMEM),
         (second, VMEM)],
        [shaped(start_block.shape), shaped((3, columns, columns))],
        work=2.0,
    )
    return residual, coefficients


def solution(mesh):
    in_specs = (
        P("row", "col"),
        P(("row", "col"), None, None),
        P(("row", "col")),
        P("row", None),
        P(("row", "col")),
        P(("row", "col"), None),
    )
    out_specs = (P(("row", "col"), None), P())
    return jax.shard_map(
        on_device, mesh=mesh, in_specs=in_specs, out_specs=out_specs, check_vma=False
    )
```

```python
import functools

import jax
import jax.numpy as jnp
from jax import lax
from jax.experimental import pallas as pl
from jax.experimental.pallas import tpu as pltpu
from jax.sharding import PartitionSpec as P


highest = lax.Precision.HIGHEST
AXES = ("row", "col")
SHIFT = 1.25
HALVES = False
FLOPS_PER_US = 5e8


def build_tile(row_correlation, row_neighbor, column_correlation, column_neighbor, coarse, weights):
    band_size = row_correlation.shape[1]
    coarse_count = coarse.shape[0] // band_size
    blocks = coarse.reshape(coarse_count, band_size, coarse_count, band_size)[
        :, :, column_neighbor, :
    ]
    mapped = jnp.einsum(
        "cakb,kbe->cake", blocks, column_correlation, preferred_element_type=jnp.float32
    ).astype(jnp.bfloat16)
    chosen = mapped[row_neighbor]
    product = jnp.einsum(
        "kai,kaje->kije", row_correlation, chosen, preferred_element_type=jnp.float32
    )
    scaled = (product * weights[:, None, :, None]).astype(jnp.bfloat16)
    return scaled.reshape(
        row_correlation.shape[0] * band_size, column_correlation.shape[0] * band_size
    )


def apply_down(kernel_tile, vectors):
    partial_value = jnp.dot(
        kernel_tile,
        lax.all_gather(vectors, "row", axis=0, tiled=True),
        preferred_element_type=jnp.float32,
    )
    return lax.psum_scatter(partial_value, "col", scatter_dimension=0, tiled=True)


def general_form(coarse_kernel, correlations, neighbor, pair_weight, energies, start_block):
    row_correlation, row_neighbor = (
        lax.all_gather(correlations, "col", axis=0, tiled=True),
        lax.all_gather(neighbor, "col", axis=0, tiled=True),
    )
    column_correlation, column_neighbor = (
        lax.all_gather(correlations, "row", axis=0, tiled=True),
        lax.all_gather(neighbor, "row", axis=0, tiled=True),
    )
    coarse_strip = lax.all_gather(coarse_kernel, "row", axis=0, tiled=True)
    coarse = lax.all_gather(coarse_strip, "col", axis=1, tiled=True)
    row_count = lax.axis_size("row")
    col_count = lax.axis_size("col")
    fine_rows = pair_weight.shape[0]
    per_device = fine_rows // col_count
    weight_grid = pair_weight.reshape(fine_rows, row_count, col_count, per_device)
    weights = lax.dynamic_index_in_dim(weight_grid, lax.axis_index("col"), 2, keepdims=False)
    weights = weights.reshape(fine_rows, row_count * per_device)
    kernel_tile = build_tile(
        row_correlation, row_neighbor, column_correlation, column_neighbor, coarse, weights
    )
    total_rows = float(start_block.shape[0] * row_count * col_count)
    first_gram = (
        lax.psum(jnp.dot(start_block.T, start_block, precision=highest), ("row", "col"))
        / total_rows
    )
    lower_first = jnp.linalg.cholesky(first_gram)
    basis = jax.scipy.linalg.solve_triangular(lower_first, start_block.T, lower=True).T
    first_term = apply_down(kernel_tile, basis.astype(jnp.bfloat16))
    image = energies[:, None] * basis + first_term
    local_projection = jnp.dot(basis.T, image, precision=highest)
    summed_projection, summed_square = lax.psum(
        (local_projection, jnp.dot(image.T, image, precision=highest)), ("row", "col")
    )
    alpha_first = summed_projection / total_rows
    remainder = image - jnp.dot(basis, alpha_first, precision=highest)
    next_gram = summed_square / total_rows - jnp.dot(alpha_first.T, alpha_first, precision=highest)
    lower_next = jnp.linalg.cholesky(next_gram)
    second = jax.scipy.linalg.solve_triangular(lower_next, remainder.T, lower=True).T
    second_term = apply_down(kernel_tile, second.astype(jnp.bfloat16))
    image_next = (
        energies[:, None] * second + second_term - jnp.dot(basis, lower_next, precision=highest)
    )
    alpha_next = (
        lax.psum(jnp.dot(second.T, image_next, precision=highest), ("row", "col")) / total_rows
    )
    residual = image_next - jnp.dot(second, alpha_next, precision=highest)
    return (residual, jnp.stack([alpha_first, lower_next, alpha_next]))


def permute(value, dims, step):
    nz, ny, nx, nc = dims
    pairs = []
    for z in range(nz):
        for y in range(ny):
            for x in range(nx):
                for c in range(nc):
                    source = ((z * ny + y) * nx + x) * nc + c
                    target = (
                        (((z + step[0]) % nz) * ny + (y + step[1]) % ny) * nx + (x + step[2]) % nx
                    ) * nc + (c + step[3]) % nc
                    pairs.append((source, target))
    return lax.ppermute(value, AXES, pairs)


def line_order(nz):
    return [0] + sorted(range(1, nz), key=lambda s: min(s, nz - s))


def gather_everywhere(block, dims, groups, halves=False):
    nz, ny, nx, nc = dims
    line = [block]
    for s in line_order(nz)[1:]:
        line.append(permute(block, dims, (s, 0, 0, 0)))
    found = {}
    for lo, hi in groups:
        own = line[lo] if hi == lo + 1 else jnp.concatenate(line[lo:hi])
        found[(0, 0, 0, lo, hi)] = own
        middle = (lo + hi) // 2
        for y, x in sorted(((y, x) for y in range(ny) for x in range(nx)), key=sum):
            if (y, x) == (0, 0):
                continue
            if halves and y and x and lo < middle:
                at = (middle - lo) * block.shape[0]
                found[(y, x, 0, lo, middle)] = permute(
                    found[(0, x, 0, lo, hi)][:at], dims, (0, y, 0, 0)
                )
                found[(y, x, 0, middle, hi)] = permute(
                    found[(y, 0, 0, lo, hi)][at:], dims, (0, 0, x, 0)
                )
            else:
                found[(y, x, 0, lo, hi)] = permute(own, dims, (0, y, x, 0))
    for y, x, _, lo, hi in list(found):
        for c in range(1, nc):
            found[(y, x, c, lo, hi)] = permute(found[(y, x, 0, lo, hi)], dims, (0, 0, 0, c))
    return list(found.values()), list(found)


def exchange(value, dims, axis, bit):
    nz, ny, nx, nc = dims
    pairs = []
    for z in range(nz):
        for y in range(ny):
            for x in range(nx):
                for c in range(nc):
                    to = [z, y, x, c]
                    to[axis] ^= bit
                    pairs.append(
                        tuple(
                            ((p[0] * ny + p[1]) * nx + p[2]) * nc + p[3]
                            for p in ((z, y, x, c), to)
                        )
                    )
    return lax.ppermute(value, AXES, pairs)


def sum_everywhere(value, dims):
    for axis in (3, 2, 0, 1):
        n = dims[axis]
        if n & (n - 1) == 0:
            bit = 1
            while bit < n:
                other = exchange(value, dims, axis, bit)
                value = value + other
                bit *= 2
        else:
            total = value
            for s in range(1, n):
                step = [0, 0, 0, 0]
                step[axis] = s
                total = total + permute(value, dims, tuple(step))
            value = total
    return value


def split(value):
    high = value.astype(jnp.bfloat16)
    low = (value - high.astype(jnp.float32)).astype(jnp.bfloat16)
    return high, low


def times(value, weight, transposed):
    high, low = split(value)
    n = value.shape[0]
    both = lax.dot_general(
        jnp.concatenate([high, low]),
        weight,
        (((1,), (1 if transposed else 0,)), ((), ())),
        preferred_element_type=jnp.float32,
    )
    return both[:n] + both[n:]


def nt(a, b):
    return lax.dot_general(
        a, b, (((1,), (1,)), ((), ())), precision=highest, preferred_element_type=jnp.float32
    )


def nn(a, b):
    return lax.dot_general(
        a, b, (((1,), (0,)), ((), ())), precision=highest, preferred_element_type=jnp.float32
    )


def first_kernel(points, neighbor, turned, correlation, payload):
    band = correlation.shape[1]
    columns = turned.shape[0]
    for p in range(points):
        u = times(turned[:, p * band : (p + 1) * band], correlation[p], True)
        payload[pl.ds(p * columns, columns), :] = u.astype(jnp.bfloat16)
    lane = lax.broadcasted_iota(jnp.int32, (16, band), 1)
    value = jnp.zeros((16, band), jnp.float32)
    for p in range(points):
        value = jnp.where(lane == p, neighbor[p].astype(jnp.float32), value)
    payload[pl.ds(points * columns, 16), :] = value.astype(jnp.bfloat16)


def wrapped(value, n):
    return lax.rem(value + 2 * n, n)


def place(geometry):
    _, ny, _, nc = geometry.dims
    row, col = lax.axis_index("row"), lax.axis_index("col")
    return row // ny, lax.rem(row, ny), col // nc, lax.rem(col, nc)


def line_step(geometry, line):
    step = jnp.int32(geometry.order[0])
    for k in range(1, len(geometry.order)):
        step = jnp.where(line == k, geometry.order[k], step)
    return step


def weigh_kernel(geometry, pieces, block_rows, with_neighbors, continued, *refs):
    dims, points, columns = geometry.dims, geometry.points, geometry.columns
    nz, ny, nx, nc = dims
    n = len(pieces)
    starts = [sum(p[4] - p[3] for p in pieces[:k]) for k in range(n)]
    u_refs, refs = refs[:n], refs[n:]
    weight, refs = refs[0], refs[1:]
    if continued:
        before, refs = refs[:2], refs[2:]
    if with_neighbors:
        acc_0, acc_1, nbs_out, nbv, nbs, sem = refs
        for index, piece in enumerate(pieces):
            for line in range(piece[4] - piece[3]):
                at = line * block_rows + points * columns
                tile = u_refs[index][pl.ds(at, 16), :].astype(jnp.float32)
                nbv[pl.ds(starts[index] + line, 1), :] = tile[0:1].astype(jnp.int32)
        copy = pltpu.make_async_copy(nbv, nbs, sem)
        copy.start()
        nbs_out[...] = nbv[...]
    else:
        nbs, acc_0, acc_1 = refs
    sums = (acc_0, acc_1)
    for k in range(2):
        sums[k][...] = before[k][...] if continued else jnp.zeros_like(sums[k])
    if with_neighbors:
        copy.wait()
    z, y, x, c = place(geometry)
    col = lax.axis_index("col")
    for index, ref in enumerate(u_refs):
        dy, dx, dc, lo, hi = pieces[index]

        def body(line, carry, ref=ref, index=index, dy=dy, dx=dx, dc=dc, lo=lo):
            device = (
                (wrapped(z - line_step(geometry, line + lo), nz) * ny + wrapped(y - dy, ny)) * nx
                + wrapped(x - dx, nx)
            ) * nc + wrapped(c - dc, nc)
            for q in range(points):
                base = pl.multiple_of(line * block_rows + q * columns, 16)
                u = ref[pl.ds(base, columns), :].astype(jnp.float32)
                j = nbs[starts[index] + line, q]
                acc = sums[q % 2]
                for p in range(points):
                    w = weight[col * points + p, device * points + q]
                    acc[j, p] += w * u
            return carry

        lax.fori_loop(0, hi - lo, body, 0)


def choose_blocks(geometry, pieces, coarse_refs, own, chosen):
    nz, ny, nx, nc = geometry.dims
    band, per_row, per_col = geometry.band, geometry.per_row, geometry.per_col
    lines = len(geometry.order)
    z, y, x, c = place(geometry)
    for p in range(geometry.points):
        owner_row = own[p] // per_row
        dz = wrapped(z - owner_row // ny, nz)
        dy = wrapped(y - lax.rem(owner_row, ny), ny)
        line = jnp.int32(0)
        for k in range(lines):
            line = jnp.where(dz == geometry.order[k], k, line)
        inner = lax.rem(own[p], per_row)
        for dx in range(nx):
            for dc in range(nc):
                owner_col = wrapped(x - dx, nx) * nc + wrapped(c - dc, nc)
                for k in range(per_col):
                    cut = slice(k * band, (k + 1) * band)
                    block = None
                    for ref, piece in zip(coarse_refs, pieces):
                        if piece[1:3] != (dx, dc):
                            continue
                        lo, hi = piece[3:]
                        at = jnp.clip(line - lo, 0, hi - lo - 1)
                        base = pl.multiple_of((at * per_row + inner) * band, 16)
                        other = ref[pl.ds(base, band), cut]
                        if block is None:
                            block = other
                        else:
                            hit = (dy == piece[0]) & (line >= lo) & (line < hi)
                            block = jnp.where(hit, other, block)
                    chosen[p, owner_col * per_col + k] = block


def image_of(acc_0, acc_1, chosen, correlation, p):
    total = times(acc_0[0, p] + acc_1[0, p], chosen[p, 0], True)
    for j in range(1, acc_0.shape[0]):
        total += times(acc_0[j, p] + acc_1[j, p], chosen[p, j], True)
    return times(total, correlation[p], False)


def first_image_kernel(geometry, pieces, count, *refs):
    n = len(pieces)
    coarse_refs = refs[:n]
    (acc_0, acc_1, own, correlation, turned, energy, chosen, payload, image, grams) = refs[n:]
    columns, band = geometry.columns, geometry.band
    choose_blocks(geometry, pieces, coarse_refs, own, chosen)
    for p in range(geometry.points):
        cut = slice(p * band, (p + 1) * band)
        value = energy[:, cut] * turned[:, cut] + image_of(acc_0, acc_1, chosen, correlation, p)
        image[:, cut] = value
        payload[pl.ds(p * columns, columns), :] = times(value, correlation[p], True).astype(
            jnp.bfloat16
        )
    pair = jnp.concatenate([turned[...], image[...]])
    grams[...] = nt(pair, pair) * (1.0 / count)


def second_image_kernel(
    geometry, count, acc_0, acc_1, chosen, correlation, first, energy, image, gram
):
    band = geometry.band
    for p in range(geometry.points):
        cut = slice(p * band, (p + 1) * band)
        image[:, cut] = energy[:, cut] * first[:, cut] + image_of(acc_0, acc_1, chosen, correlation, p)
    gram[...] = nt(first[...], image[...]) * (1.0 / count)


def eliminate(work, begin, end):
    rows = lax.broadcasted_iota(jnp.int32, (work.shape[0], 1), 0)
    for k in range(begin, end):
        scale = lax.rsqrt(work[k : k + 1, k : k + 1])
        pivot = work[k : k + 1, :] * scale
        column = jnp.where(rows > k, work[:, k : k + 1] * scale, 0.0)
        work = jnp.where(rows == k, pivot, work - column * pivot)
    return work


def unit(m):
    return (
        lax.broadcasted_iota(jnp.int32, (m, m), 0) == lax.broadcasted_iota(jnp.int32, (m, m), 1)
    ).astype(jnp.float32)


def eliminate_kernel_1(joint, out):
    m = joint.shape[0] // 2
    work = jnp.concatenate([joint[:m, :m], unit(m), joint[:m, m:]], axis=1)
    out[...] = eliminate(work, 0, m // 2)


def eliminate_kernel_2(joint, given, out, schur):
    m = joint.shape[0] // 2
    work = eliminate(given[...], m // 2, m)
    out[...] = work
    z1 = work[:, 2 * m :]
    schur[...] = jnp.concatenate([joint[m:, m:] - nn(z1.T, z1), unit(m)], axis=1)


def eliminate_kernel_3(given, out):
    m = given.shape[0]
    out[...] = eliminate(given[...], 0, m // 2)


def eliminate_kernel_4(joint, one, given, first_two, parts):
    m = given.shape[0]
    work = eliminate(given[...], m // 2, m)
    keep = lax.broadcasted_iota(jnp.int32, (m, m), 0) <= lax.broadcasted_iota(jnp.int32, (m, m), 1)
    upper = jnp.where(keep, work[:, :m], 0.0)
    t_x = work[:, m:]
    inverse_first, z1 = one[:, m : 2 * m], one[:, 2 * m :]
    g01, g11 = joint[:m, m:], joint[m:, m:]
    first_two[0] = nt(z1, inverse_first) + SHIFT * unit(m)
    first_two[1] = nn(inverse_first, upper.T)
    t_s = -nn(t_x, nn(z1.T, inverse_first))
    p_s = nn(t_s, g01) + nn(t_x, g11)
    parts[0] = t_s
    parts[1] = t_x
    parts[2] = nt(p_s, t_s) + nt(nn(t_s, g11), t_x)
    parts[3] = nn(nn(upper, inverse_first.T), inverse_first)


def last_kernel(*refs):
    n = len(refs) - 7
    (first_two, parts, turned, first, second, residual, coefficients) = refs[n:]
    g12 = refs[0][...]
    for k in range(1, n):
        g12 += refs[k][...]
    m = g12.shape[0]
    t_s, t_x = parts[0], parts[1]
    alpha_next = parts[2] + nt(nn(t_x, g12), t_x)
    on_start = -parts[3] - nn(alpha_next, t_s)
    on_first = t_s - nn(alpha_next, t_x)
    coefficients[0] = first_two[0]
    coefficients[1] = first_two[1]
    coefficients[2] = alpha_next + SHIFT * unit(m)
    factors = jnp.concatenate([on_start, on_first, t_x], axis=1)
    residual[...] = nn(factors, jnp.concatenate([turned[...], first[...], second[...]]))


VMEM = pl.BlockSpec(memory_space=pltpu.VMEM)
SMEM = pl.BlockSpec(memory_space=pltpu.SMEM)


class Geometry:
    def __init__(self, **values):
        self.__dict__.update(values)


def shaped(shape, dtype=jnp.float32):
    return jax.ShapeDtypeStruct(shape, dtype)


def call(kernel, inputs, outputs, scratch=(), work=0.0, aliases=None):
    return pl.pallas_call(
        kernel,
        in_specs=[spec for _, spec in inputs],
        out_shape=outputs,
        out_specs=[VMEM] * len(outputs),
        scratch_shapes=list(scratch),
        input_output_aliases=aliases or {},
        cost_estimate=pl.CostEstimate(
            flops=int(work * FLOPS_PER_US), bytes_accessed=0, transcendentals=0
        ),
        compiler_params=pltpu.CompilerParams(vmem_limit_bytes=48 * 2**20),
    )(*[value for value, _ in inputs])


def weigh(geometry, arrays, pieces, block_rows, weight, neighbors, before=None):
    shape = (geometry.coarse_count, geometry.points, geometry.columns, geometry.band)
    inputs = [(a, VMEM) for a in arrays] + [(weight, SMEM)]
    at = len(inputs)
    if before is not None:
        inputs += [(b, VMEM) for b in before]
    outputs = [shaped(shape), shaped(shape)]
    scratch = []
    count = sum(piece[4] - piece[3] for piece in pieces)
    if neighbors is None:
        outputs.append(shaped((count, geometry.band), jnp.int32))
        scratch = [
            pltpu.VMEM((count, geometry.band), jnp.int32),
            pltpu.SMEM((count, geometry.band), jnp.int32),
            pltpu.SemaphoreType.DMA,
        ]
    else:
        inputs.append((neighbors, SMEM))
    found = call(
        functools.partial(
            weigh_kernel, geometry, pieces, block_rows, neighbors is None, before is not None
        ),
        inputs,
        outputs,
        scratch,
        work=1.0 * len(arrays) / 2,
        aliases={at: 0, at + 1: 1} if before is not None else None,
    )
    return found[:2], found[2:]


def on_device(coarse_kernel, correlations, neighbor, pair_weight, energies, start_block):
    rows, cols = lax.axis_size("row"), lax.axis_size("col")
    points, band, _ = correlations.shape
    columns = start_block.shape[1]
    if rows % 2 or cols % 2 or coarse_kernel.shape[0] % band or coarse_kernel.shape[1] % band:
        return general_form(
            coarse_kernel, correlations, neighbor, pair_weight, energies, start_block
        )
    dims = (rows // 2, 2, cols // 2, 2)
    order = line_order(dims[0])
    per_row, per_col = coarse_kernel.shape[0] // band, coarse_kernel.shape[1] // band
    geometry = Geometry(
        dims=dims, order=order, points=points, columns=columns, band=band,
        per_row=per_row, per_col=per_col, coarse_count=per_row * rows,
    )
    count = float(start_block.shape[0] * rows * cols)
    half = points * columns
    turned = start_block.T
    (payload,) = call(
        functools.partial(first_kernel, points),
        [(neighbor, SMEM), (turned, VMEM), (correlations, VMEM)],
        [shaped((half + 16, band), jnp.bfloat16)],
        work=1.0,
    )
    shifted = energies[None, :] - SHIFT

    nz = dims[0]
    apart = [(0, 1), (1, nz)] if nz > 1 else [(0, 1)]
    u, pieces = gather_everywhere(payload, dims, apart)
    coarse, coarse_pieces = gather_everywhere(coarse_kernel, dims, [(0, nz)], HALVES)

    def group_of(piece):
        y, x, _, lo, _ = piece
        return 0 if lo == 0 or (y, x) == (0, 0) else 1 if y == 0 else 2

    groups = [[k for k, p in enumerate(pieces) if group_of(p) == g] for g in range(3)]
    groups = [group for group in groups if group]
    acc, neighbors = None, []
    for group in groups:
        acc, found = weigh(
            geometry, [u[k] for k in group], [pieces[k] for k in group], half + 16,
            pair_weight, None, acc,
        )
        neighbors.append(found[0])
    own = neighbors[0][0, :points]
    coarse_count = geometry.coarse_count
    chosen, payload, first, joint = call(
        functools.partial(first_image_kernel, geometry, coarse_pieces, count),
        [(a, VMEM) for a in coarse]
        + [(acc[0], VMEM), (acc[1], VMEM), (own, SMEM), (correlations, VMEM), (turned, VMEM), (shifted, VMEM)],
        [
            shaped((points, coarse_count, band, band), jnp.bfloat16),
            shaped((half, band), jnp.bfloat16),
            shaped(turned.shape),
            shaped((2 * columns, 2 * columns)),
        ],
        work=3.0,
    )
    u, _ = gather_everywhere(payload, dims, apart)
    joint = sum_everywhere(joint, dims)
    acc = None
    for group, found in zip(groups, neighbors):
        acc, _ = weigh(
            geometry, [u[k] for k in group], [pieces[k] for k in group], half,
            pair_weight, found, acc,
        )
    second, g12 = call(
        functools.partial(second_image_kernel, geometry, count),
        [(acc[0], VMEM), (acc[1], VMEM), (chosen, VMEM), (correlations, VMEM), (first, VMEM), (shifted, VMEM)],
        [shaped(turned.shape), shaped((columns, columns))],
        work=3.0,
    )
    m = columns
    (one,) = call(eliminate_kernel_1, [(joint, VMEM)], [shaped((m, 3 * m))], work=3.0)
    one, schur = call(
        eliminate_kernel_2, [(joint, VMEM), (one, VMEM)],
        [shaped((m, 3 * m)), shaped((m, 2 * m))], work=3.0,
    )
    (two,) = call(eliminate_kernel_3, [(schur, VMEM)], [shaped((m, 2 * m))], work=3.0)
    first_two, parts = call(
        eliminate_kernel_4, [(joint, VMEM), (one, VMEM), (two, VMEM)],
        [shaped((2, m, m)), shaped((4, m, m))], work=3.0,
    )
    g12 = sum_everywhere(g12, dims)
    residual, coefficients = call(
        last_kernel,
        [(g12, VMEM), (first_two, VMEM), (parts, VMEM), (turned, VMEM), (first, VMEM),
         (second, VMEM)],
        [shaped(turned.shape), shaped((3, columns, columns))],
        work=2.0,
    )
    return residual.T, coefficients


def solution(mesh):
    in_specs = (
        P("row", "col"),
        P(("row", "col"), None, None),
        P(("row", "col")),
        P("row", None),
        P(("row", "col")),
        P(("row", "col"), None),
    )
    out_specs = (P(("row", "col"), None), P())
    return jax.shard_map(
        on_device, mesh=mesh, in_specs=in_specs, out_specs=out_specs, check_vma=False
    )
```

```python
import functools

import jax
import jax.numpy as jnp
from jax import lax
from jax.experimental import pallas as pl
from jax.experimental.pallas import tpu as pltpu
from jax.sharding import PartitionSpec as P


highest = lax.Precision.HIGHEST
AXES = ("row", "col")
SHIFT = 1.25
HALVES = False
FLOPS_PER_US = 5e8


def build_tile(row_correlation, row_neighbor, column_correlation, column_neighbor, coarse, weights):
    band_size = row_correlation.shape[1]
    coarse_count = coarse.shape[0] // band_size
    blocks = coarse.reshape(coarse_count, band_size, coarse_count, band_size)[
        :, :, column_neighbor, :
    ]
    mapped = jnp.einsum(
        "cakb,kbe->cake", blocks, column_correlation, preferred_element_type=jnp.float32
    ).astype(jnp.bfloat16)
    chosen = mapped[row_neighbor]
    product = jnp.einsum(
        "kai,kaje->kije", row_correlation, chosen, preferred_element_type=jnp.float32
    )
    scaled = (product * weights[:, None, :, None]).astype(jnp.bfloat16)
    return scaled.reshape(
        row_correlation.shape[0] * band_size, column_correlation.shape[0] * band_size
    )


def apply_down(kernel_tile, vectors):
    partial_value = jnp.dot(
        kernel_tile,
        lax.all_gather(vectors, "row", axis=0, tiled=True),
        preferred_element_type=jnp.float32,
    )
    return lax.psum_scatter(partial_value, "col", scatter_dimension=0, tiled=True)


def general_form(coarse_kernel, correlations, neighbor, pair_weight, energies, start_block):
    row_correlation, row_neighbor = (
        lax.all_gather(correlations, "col", axis=0, tiled=True),
        lax.all_gather(neighbor, "col", axis=0, tiled=True),
    )
    column_correlation, column_neighbor = (
        lax.all_gather(correlations, "row", axis=0, tiled=True),
        lax.all_gather(neighbor, "row", axis=0, tiled=True),
    )
    coarse_strip = lax.all_gather(coarse_kernel, "row", axis=0, tiled=True)
    coarse = lax.all_gather(coarse_strip, "col", axis=1, tiled=True)
    row_count = lax.axis_size("row")
    col_count = lax.axis_size("col")
    fine_rows = pair_weight.shape[0]
    per_device = fine_rows // col_count
    weight_grid = pair_weight.reshape(fine_rows, row_count, col_count, per_device)
    weights = lax.dynamic_index_in_dim(weight_grid, lax.axis_index("col"), 2, keepdims=False)
    weights = weights.reshape(fine_rows, row_count * per_device)
    kernel_tile = build_tile(
        row_correlation, row_neighbor, column_correlation, column_neighbor, coarse, weights
    )
    total_rows = float(start_block.shape[0] * row_count * col_count)
    first_gram = (
        lax.psum(jnp.dot(start_block.T, start_block, precision=highest), ("row", "col"))
        / total_rows
    )
    lower_first = jnp.linalg.cholesky(first_gram)
    basis = jax.scipy.linalg.solve_triangular(lower_first, start_block.T, lower=True).T
    first_term = apply_down(kernel_tile, basis.astype(jnp.bfloat16))
    image = energies[:, None] * basis + first_term
    local_projection = jnp.dot(basis.T, image, precision=highest)
    summed_projection, summed_square = lax.psum(
        (local_projection, jnp.dot(image.T, image, precision=highest)), ("row", "col")
    )
    alpha_first = summed_projection / total_rows
    remainder = image - jnp.dot(basis, alpha_first, precision=highest)
    next_gram = summed_square / total_rows - jnp.dot(alpha_first.T, alpha_first, precision=highest)
    lower_next = jnp.linalg.cholesky(next_gram)
    second = jax.scipy.linalg.solve_triangular(lower_next, remainder.T, lower=True).T
    second_term = apply_down(kernel_tile, second.astype(jnp.bfloat16))
    image_next = (
        energies[:, None] * second + second_term - jnp.dot(basis, lower_next, precision=highest)
    )
    alpha_next = (
        lax.psum(jnp.dot(second.T, image_next, precision=highest), ("row", "col")) / total_rows
    )
    residual = image_next - jnp.dot(second, alpha_next, precision=highest)
    return (residual, jnp.stack([alpha_first, lower_next, alpha_next]))


def permute(value, dims, step):
    nz, ny, nx, nc = dims
    pairs = []
    for z in range(nz):
        for y in range(ny):
            for x in range(nx):
                for c in range(nc):
                    source = ((z * ny + y) * nx + x) * nc + c
                    target = (
                        (((z + step[0]) % nz) * ny + (y + step[1]) % ny) * nx + (x + step[2]) % nx
                    ) * nc + (c + step[3]) % nc
                    pairs.append((source, target))
    return lax.ppermute(value, AXES, pairs)


def line_order(nz):
    return [0] + sorted(range(1, nz), key=lambda s: min(s, nz - s))


def gather_everywhere(block, dims, groups, halves=False):
    nz, ny, nx, nc = dims
    line = [block]
    for s in line_order(nz)[1:]:
        line.append(permute(block, dims, (s, 0, 0, 0)))
    found = {}
    for lo, hi in groups:
        own = line[lo] if hi == lo + 1 else jnp.concatenate(line[lo:hi])
        found[(0, 0, 0, lo, hi)] = own
        middle = (lo + hi) // 2
        for y, x in sorted(((y, x) for y in range(ny) for x in range(nx)), key=sum):
            if (y, x) == (0, 0):
                continue
            if halves and y and x and lo < middle:
                at = (middle - lo) * block.shape[0]
                found[(y, x, 0, lo, middle)] = permute(
                    found[(0, x, 0, lo, hi)][:at], dims, (0, y, 0, 0)
                )
                found[(y, x, 0, middle, hi)] = permute(
                    found[(y, 0, 0, lo, hi)][at:], dims, (0, 0, x, 0)
                )
            else:
                found[(y, x, 0, lo, hi)] = permute(own, dims, (0, y, x, 0))
    for y, x, _, lo, hi in list(found):
        for c in range(1, nc):
            found[(y, x, c, lo, hi)] = permute(found[(y, x, 0, lo, hi)], dims, (0, 0, 0, c))
    return list(found.values()), list(found)


def exchange(value, dims, axis, bit):
    nz, ny, nx, nc = dims
    pairs = []
    for z in range(nz):
        for y in range(ny):
            for x in range(nx):
                for c in range(nc):
                    to = [z, y, x, c]
                    to[axis] ^= bit
                    pairs.append(
                        tuple(
                            ((p[0] * ny + p[1]) * nx + p[2]) * nc + p[3]
                            for p in ((z, y, x, c), to)
                        )
                    )
    return lax.ppermute(value, AXES, pairs)


def sum_everywhere(value, dims):
    for axis in (3, 2, 0, 1):
        n = dims[axis]
        if n & (n - 1) == 0:
            bit = 1
            while bit < n:
                other = exchange(value, dims, axis, bit)
                value = value + other
                bit *= 2
        else:
            total = value
            for s in range(1, n):
                step = [0, 0, 0, 0]
                step[axis] = s
                total = total + permute(value, dims, tuple(step))
            value = total
    return value


def split(value):
    high = value.astype(jnp.bfloat16)
    low = (value - high.astype(jnp.float32)).astype(jnp.bfloat16)
    return high, low


def times(value, weight, transposed):
    high, low = split(value)
    n = value.shape[0]
    both = lax.dot_general(
        jnp.concatenate([high, low]),
        weight,
        (((1,), (1 if transposed else 0,)), ((), ())),
        preferred_element_type=jnp.float32,
    )
    return both[:n] + both[n:]


def nt(a, b):
    return lax.dot_general(
        a, b, (((1,), (1,)), ((), ())), precision=highest, preferred_element_type=jnp.float32
    )


def nn(a, b):
    return lax.dot_general(
        a, b, (((1,), (0,)), ((), ())), precision=highest, preferred_element_type=jnp.float32
    )


def first_kernel(points, neighbor, turned, correlation, payload):
    band = correlation.shape[1]
    columns = turned.shape[0]
    for p in range(points):
        u = times(turned[:, p * band : (p + 1) * band], correlation[p], True)
        payload[pl.ds(p * columns, columns), :] = u.astype(jnp.bfloat16)
    lane = lax.rem(lax.broadcasted_iota(jnp.int32, (16, band), 1), points)
    value = jnp.zeros((16, band), jnp.float32)
    for p in range(points):
        value = jnp.where(lane == p, neighbor[p].astype(jnp.float32), value)
    payload[pl.ds(points * columns, 16), :] = value.astype(jnp.bfloat16)


def wrapped(value, n):
    return lax.rem(value + 2 * n, n)


def place(geometry):
    _, ny, _, nc = geometry.dims
    row, col = lax.axis_index("row"), lax.axis_index("col")
    return row // ny, lax.rem(row, ny), col // nc, lax.rem(col, nc)


def line_step(geometry, line):
    step = jnp.int32(geometry.order[0])
    for k in range(1, len(geometry.order)):
        step = jnp.where(line == k, geometry.order[k], step)
    return step


def weigh_kernel(geometry, pieces, block_rows, with_neighbors, continued, *refs):
    dims, points, columns, band = geometry.dims, geometry.points, geometry.columns, geometry.band
    nz, ny, nx, nc = dims
    n = len(pieces)
    starts = [sum(p[4] - p[3] for p in pieces[:k]) for k in range(n)]
    u_refs, refs = refs[:n], refs[n:]
    weight, refs = refs[0], refs[1:]
    if continued:
        before, refs = refs[:2], refs[2:]
    if with_neighbors:
        acc_0, acc_1, nbs_out, nbv, nbs, sem = refs
        per = band // points
        lane = lax.broadcasted_iota(jnp.int32, (16, band), 1) // points
        rows = [jnp.zeros((16, band), jnp.float32) for _ in range(nbv.shape[0])]
        for index, piece in enumerate(pieces):
            for line in range(piece[4] - piece[3]):
                at = line * block_rows + points * columns
                tile = u_refs[index][pl.ds(at, 16), :].astype(jnp.float32)
                k = starts[index] + line
                rows[k // per] = jnp.where(lane == k % per, tile, rows[k // per])
        for k, row in enumerate(rows):
            nbv[pl.ds(k, 1), :] = row[0:1].astype(jnp.int32)
        copy = pltpu.make_async_copy(nbv, nbs, sem)
        copy.start()
        nbs_out[...] = nbv[...]
    else:
        nbs, acc_0, acc_1 = refs
    sums = (acc_0, acc_1)
    for k in range(2):
        sums[k][...] = before[k][...] if continued else jnp.zeros_like(sums[k])
    if with_neighbors:
        copy.wait()
    z, y, x, c = place(geometry)
    per = band // points
    for index, ref in enumerate(u_refs):
        dy, dx, dc, lo, hi = pieces[index]

        def body(line, carry, ref=ref, index=index, dy=dy, dx=dx, dc=dc, lo=lo):
            device = (
                (wrapped(z - line_step(geometry, line + lo), nz) * ny + wrapped(y - dy, ny)) * nx
                + wrapped(x - dx, nx)
            ) * nc + wrapped(c - dc, nc)
            for q in range(points):
                base = pl.multiple_of(line * block_rows + q * columns, 16)
                u = ref[pl.ds(base, columns), :].astype(jnp.float32)
                k = starts[index] + line
                j = nbs[k // per, lax.rem(k, per) * points + q]
                acc = sums[q % 2]
                for p in range(points):
                    w = weight[p, device * points + q]
                    acc[j, p] += w * u
            return carry

        lax.fori_loop(0, hi - lo, body, 0)


def choose_blocks(geometry, pieces, coarse_refs, own, chosen):
    nz, ny, nx, nc = geometry.dims
    band, per_row, per_col = geometry.band, geometry.per_row, geometry.per_col
    lines = len(geometry.order)
    z, y, x, c = place(geometry)
    for p in range(geometry.points):
        owner_row = own[p] // per_row
        dz = wrapped(z - owner_row // ny, nz)
        dy = wrapped(y - lax.rem(owner_row, ny), ny)
        line = jnp.int32(0)
        for k in range(lines):
            line = jnp.where(dz == geometry.order[k], k, line)
        inner = lax.rem(own[p], per_row)
        for dx in range(nx):
            for dc in range(nc):
                owner_col = wrapped(x - dx, nx) * nc + wrapped(c - dc, nc)
                for k in range(per_col):
                    cut = slice(k * band, (k + 1) * band)
                    block = None
                    for ref, piece in zip(coarse_refs, pieces):
                        if piece[1:3] != (dx, dc):
                            continue
                        lo, hi = piece[3:]
                        at = jnp.clip(line - lo, 0, hi - lo - 1)
                        base = pl.multiple_of((at * per_row + inner) * band, 16)
                        other = ref[pl.ds(base, band), cut]
                        if block is None:
                            block = other
                        else:
                            hit = (dy == piece[0]) & (line >= lo) & (line < hi)
                            block = jnp.where(hit, other, block)
                    chosen[p, owner_col * per_col + k] = block


def image_of(acc_0, acc_1, chosen, correlation, p):
    total = times(acc_0[0, p] + acc_1[0, p], chosen[p, 0], True)
    for j in range(1, acc_0.shape[0]):
        total += times(acc_0[j, p] + acc_1[j, p], chosen[p, j], True)
    return times(total, correlation[p], False)


def first_image_kernel(geometry, pieces, *refs):
    n = len(pieces)
    coarse_refs = refs[:n]
    (acc_0, acc_1, own, correlation, turned, energy, chosen, payload, image) = refs[n:]
    columns, band = geometry.columns, geometry.band
    choose_blocks(geometry, pieces, coarse_refs, own, chosen)
    for p in range(geometry.points):
        cut = slice(p * band, (p + 1) * band)
        value = energy[:, cut] * turned[:, cut] + image_of(acc_0, acc_1, chosen, correlation, p)
        image[:, cut] = value
        payload[pl.ds(p * columns, columns), :] = times(value, correlation[p], True).astype(
            jnp.bfloat16
        )


def gram_kernel(count, turned, image, grams):
    pair = jnp.concatenate([turned[...], image[...]])
    grams[...] = nt(pair, pair) * (1.0 / count)


def second_image_kernel(
    geometry, count, acc_0, acc_1, chosen, correlation, first, energy, image, gram
):
    band = geometry.band
    for p in range(geometry.points):
        cut = slice(p * band, (p + 1) * band)
        image[:, cut] = energy[:, cut] * first[:, cut] + image_of(acc_0, acc_1, chosen, correlation, p)
    gram[...] = nt(first[...], image[...]) * (1.0 / count)


def eliminate(work, begin, end):
    rows = lax.broadcasted_iota(jnp.int32, (work.shape[0], 1), 0)
    for k in range(begin, end):
        scale = lax.rsqrt(work[k : k + 1, k : k + 1])
        pivot = work[k : k + 1, :] * scale
        column = jnp.where(rows > k, work[:, k : k + 1] * scale, 0.0)
        work = jnp.where(rows == k, pivot, work - column * pivot)
    return work


def unit(m):
    return (
        lax.broadcasted_iota(jnp.int32, (m, m), 0) == lax.broadcasted_iota(jnp.int32, (m, m), 1)
    ).astype(jnp.float32)


def eliminate_kernel_1(joint, out):
    m = joint.shape[0] // 2
    work = jnp.concatenate([joint[:m, :m], unit(m), joint[:m, m:]], axis=1)
    out[...] = eliminate(work, 0, m // 2)


def eliminate_kernel_2(joint, given, out, schur):
    m = joint.shape[0] // 2
    work = eliminate(given[...], m // 2, m)
    out[...] = work
    z1 = work[:, 2 * m :]
    schur[...] = jnp.concatenate([joint[m:, m:] - nn(z1.T, z1), unit(m)], axis=1)


def eliminate_kernel_3(given, out):
    m = given.shape[0]
    out[...] = eliminate(given[...], 0, m // 2)


def eliminate_kernel_4(joint, one, given, first_two, parts):
    m = given.shape[0]
    work = eliminate(given[...], m // 2, m)
    keep = lax.broadcasted_iota(jnp.int32, (m, m), 0) <= lax.broadcasted_iota(jnp.int32, (m, m), 1)
    upper = jnp.where(keep, work[:, :m], 0.0)
    t_x = work[:, m:]
    inverse_first, z1 = one[:, m : 2 * m], one[:, 2 * m :]
    g01, g11 = joint[:m, m:], joint[m:, m:]
    first_two[0] = nt(z1, inverse_first) + SHIFT * unit(m)
    first_two[1] = nn(inverse_first, upper.T)
    t_s = -nn(t_x, nn(z1.T, inverse_first))
    p_s = nn(t_s, g01) + nn(t_x, g11)
    parts[0] = t_s
    parts[1] = t_x
    parts[2] = nt(p_s, t_s) + nt(nn(t_s, g11), t_x)
    parts[3] = nn(nn(upper, inverse_first.T), inverse_first)


def last_kernel(*refs):
    n = len(refs) - 7
    (first_two, parts, turned, first, second, residual, coefficients) = refs[n:]
    g12 = refs[0][...]
    for k in range(1, n):
        g12 += refs[k][...]
    m = g12.shape[0]
    t_s, t_x = parts[0], parts[1]
    alpha_next = parts[2] + nt(nn(t_x, g12), t_x)
    on_start = -parts[3] - nn(alpha_next, t_s)
    on_first = t_s - nn(alpha_next, t_x)
    coefficients[0] = first_two[0]
    coefficients[1] = first_two[1]
    coefficients[2] = alpha_next + SHIFT * unit(m)
    factors = jnp.concatenate([on_start, on_first, t_x], axis=1)
    residual[...] = nn(factors, jnp.concatenate([turned[...], first[...], second[...]]))


VMEM = pl.BlockSpec(memory_space=pltpu.VMEM)
SMEM = pl.BlockSpec(memory_space=pltpu.SMEM)


class Geometry:
    def __init__(self, **values):
        self.__dict__.update(values)


def shaped(shape, dtype=jnp.float32):
    return jax.ShapeDtypeStruct(shape, dtype)


def call(kernel, inputs, outputs, scratch=(), work=0.0, aliases=None):
    return pl.pallas_call(
        kernel,
        in_specs=[spec for _, spec in inputs],
        out_shape=outputs,
        out_specs=[VMEM] * len(outputs),
        scratch_shapes=list(scratch),
        input_output_aliases=aliases or {},
        cost_estimate=pl.CostEstimate(
            flops=int(work * FLOPS_PER_US), bytes_accessed=0, transcendentals=0
        ),
        compiler_params=pltpu.CompilerParams(vmem_limit_bytes=48 * 2**20),
    )(*[value for value, _ in inputs])


def weigh(geometry, arrays, pieces, block_rows, weight, neighbors, before=None):
    shape = (geometry.coarse_count, geometry.points, geometry.columns, geometry.band)
    inputs = [(a, VMEM) for a in arrays] + [(weight, SMEM)]
    at = len(inputs)
    if before is not None:
        inputs += [(b, VMEM) for b in before]
    outputs = [shaped(shape), shaped(shape)]
    scratch = []
    blocks = sum(piece[4] - piece[3] for piece in pieces)
    count = pl.cdiv(blocks, geometry.band // geometry.points)
    if neighbors is None:
        outputs.append(shaped((count, geometry.band), jnp.int32))
        scratch = [
            pltpu.VMEM((count, geometry.band), jnp.int32),
            pltpu.SMEM((count, geometry.band), jnp.int32),
            pltpu.SemaphoreType.DMA,
        ]
    else:
        inputs.append((neighbors, SMEM))
    found = call(
        functools.partial(
            weigh_kernel, geometry, pieces, block_rows, neighbors is None, before is not None
        ),
        inputs,
        outputs,
        scratch,
        work=1.0 * len(arrays) / 2,
        aliases={at: 0, at + 1: 1} if before is not None else None,
    )
    return found[:2], found[2:]


def on_device(coarse_kernel, correlations, neighbor, pair_weight, energies, start_block):
    rows, cols = lax.axis_size("row"), lax.axis_size("col")
    points, band, _ = correlations.shape
    columns = start_block.shape[1]
    if rows % 2 or cols % 2 or coarse_kernel.shape[0] % band or coarse_kernel.shape[1] % band or band % points:
        return general_form(
            coarse_kernel, correlations, neighbor, pair_weight, energies, start_block
        )
    dims = (rows // 2, 2, cols // 2, 2)
    order = line_order(dims[0])
    per_row, per_col = coarse_kernel.shape[0] // band, coarse_kernel.shape[1] // band
    geometry = Geometry(
        dims=dims, order=order, points=points, columns=columns, band=band,
        per_row=per_row, per_col=per_col, coarse_count=per_row * rows,
    )
    count = float(start_block.shape[0] * rows * cols)
    half = points * columns
    turned = start_block.T
    own_weight = lax.dynamic_slice_in_dim(
        pair_weight, lax.axis_index("col") * points, points, axis=0
    )
    (payload,) = call(
        functools.partial(first_kernel, points),
        [(neighbor, SMEM), (turned, VMEM), (correlations, VMEM)],
        [shaped((half + 16, band), jnp.bfloat16)],
        work=1.0,
    )
    shifted = energies[None, :] - SHIFT

    nz = dims[0]
    apart = [(0, 1), (1, nz)] if nz > 1 else [(0, 1)]
    u, pieces = gather_everywhere(payload, dims, apart)
    coarse, coarse_pieces = gather_everywhere(coarse_kernel, dims, [(0, nz)], HALVES)

    def group_of(piece):
        y, x, _, lo, _ = piece
        return 0 if lo == 0 or (y, x) == (0, 0) else 1 if y == 0 else 2

    groups = [[k for k, p in enumerate(pieces) if group_of(p) == g] for g in range(3)]
    groups = [group for group in groups if group]
    acc, neighbors = None, []
    for group in groups:
        acc, found = weigh(
            geometry, [u[k] for k in group], [pieces[k] for k in group], half + 16,
            own_weight, None, acc,
        )
        neighbors.append(found[0])
    own = neighbors[0][0, :points]
    coarse_count = geometry.coarse_count
    chosen, payload, first = call(
        functools.partial(first_image_kernel, geometry, coarse_pieces),
        [(a, VMEM) for a in coarse]
        + [(acc[0], VMEM), (acc[1], VMEM), (own, SMEM), (correlations, VMEM), (turned, VMEM), (shifted, VMEM)],
        [
            shaped((points, coarse_count, band, band), jnp.bfloat16),
            shaped((half, band), jnp.bfloat16),
            shaped(turned.shape),
        ],
        work=3.0,
    )
    (joint,) = call(
        functools.partial(gram_kernel, count),
        [(turned, VMEM), (first, VMEM)],
        [shaped((2 * columns, 2 * columns))],
        work=1.0,
    )
    u, _ = gather_everywhere(payload, dims, apart)
    joint = sum_everywhere(joint, dims)
    acc = None
    for group, found in zip(groups, neighbors):
        acc, _ = weigh(
            geometry, [u[k] for k in group], [pieces[k] for k in group], half,
            own_weight, found, acc,
        )
    second, g12 = call(
        functools.partial(second_image_kernel, geometry, count),
        [(acc[0], VMEM), (acc[1], VMEM), (chosen, VMEM), (correlations, VMEM), (first, VMEM), (shifted, VMEM)],
        [shaped(turned.shape), shaped((columns, columns))],
        work=3.0,
    )
    m = columns
    (one,) = call(eliminate_kernel_1, [(joint, VMEM)], [shaped((m, 3 * m))], work=3.0)
    one, schur = call(
        eliminate_kernel_2, [(joint, VMEM), (one, VMEM)],
        [shaped((m, 3 * m)), shaped((m, 2 * m))], work=3.0,
    )
    (two,) = call(eliminate_kernel_3, [(schur, VMEM)], [shaped((m, 2 * m))], work=3.0)
    first_two, parts = call(
        eliminate_kernel_4, [(joint, VMEM), (one, VMEM), (two, VMEM)],
        [shaped((2, m, m)), shaped((4, m, m))], work=3.0,
    )
    g12 = sum_everywhere(g12, dims)
    residual, coefficients = call(
        last_kernel,
        [(g12, VMEM), (first_two, VMEM), (parts, VMEM), (turned, VMEM), (first, VMEM),
         (second, VMEM)],
        [shaped(turned.shape), shaped((3, columns, columns))],
        work=2.0,
    )
    return residual.T, coefficients


def solution(mesh):
    in_specs = (
        P("row", "col"),
        P(("row", "col"), None, None),
        P(("row", "col")),
        P("row", None),
        P(("row", "col")),
        P(("row", "col"), None),
    )
    out_specs = (P(("row", "col"), None), P())
    return jax.shard_map(
        on_device, mesh=mesh, in_specs=in_specs, out_specs=out_specs, check_vma=False
    )
```

```python
import functools

import jax
import jax.numpy as jnp
from jax import lax
from jax.experimental import pallas as pl
from jax.experimental.pallas import tpu as pltpu
from jax.sharding import PartitionSpec as P


highest = lax.Precision.HIGHEST
AXES = ("row", "col")
GRID = "zyxc"
SHIFT = 1.25
HALVES = False
FLOPS_PER_US = 5e8


def build_tile(row_correlation, row_neighbor, column_correlation, column_neighbor, coarse, weights):
    band_size = row_correlation.shape[1]
    coarse_count = coarse.shape[0] // band_size
    blocks = coarse.reshape(coarse_count, band_size, coarse_count, band_size)[
        :, :, column_neighbor, :
    ]
    mapped = jnp.einsum(
        "cakb,kbe->cake", blocks, column_correlation, preferred_element_type=jnp.float32
    ).astype(jnp.bfloat16)
    chosen = mapped[row_neighbor]
    product = jnp.einsum(
        "kai,kaje->kije", row_correlation, chosen, preferred_element_type=jnp.float32
    )
    scaled = (product * weights[:, None, :, None]).astype(jnp.bfloat16)
    return scaled.reshape(
        row_correlation.shape[0] * band_size, column_correlation.shape[0] * band_size
    )


def apply_down(kernel_tile, vectors):
    partial_value = jnp.dot(
        kernel_tile,
        lax.all_gather(vectors, "row", axis=0, tiled=True),
        preferred_element_type=jnp.float32,
    )
    return lax.psum_scatter(partial_value, "col", scatter_dimension=0, tiled=True)


def general_form(coarse_kernel, correlations, neighbor, pair_weight, energies, start_block):
    row_correlation, row_neighbor = (
        lax.all_gather(correlations, "col", axis=0, tiled=True),
        lax.all_gather(neighbor, "col", axis=0, tiled=True),
    )
    column_correlation, column_neighbor = (
        lax.all_gather(correlations, "row", axis=0, tiled=True),
        lax.all_gather(neighbor, "row", axis=0, tiled=True),
    )
    coarse_strip = lax.all_gather(coarse_kernel, "row", axis=0, tiled=True)
    coarse = lax.all_gather(coarse_strip, "col", axis=1, tiled=True)
    row_count = lax.axis_size("row")
    col_count = lax.axis_size("col")
    fine_rows = pair_weight.shape[0]
    per_device = fine_rows // col_count
    weight_grid = pair_weight.reshape(fine_rows, row_count, col_count, per_device)
    weights = lax.dynamic_index_in_dim(weight_grid, lax.axis_index("col"), 2, keepdims=False)
    weights = weights.reshape(fine_rows, row_count * per_device)
    kernel_tile = build_tile(
        row_correlation, row_neighbor, column_correlation, column_neighbor, coarse, weights
    )
    total_rows = float(start_block.shape[0] * row_count * col_count)
    first_gram = (
        lax.psum(jnp.dot(start_block.T, start_block, precision=highest), ("row", "col"))
        / total_rows
    )
    lower_first = jnp.linalg.cholesky(first_gram)
    basis = jax.scipy.linalg.solve_triangular(lower_first, start_block.T, lower=True).T
    first_term = apply_down(kernel_tile, basis.astype(jnp.bfloat16))
    image = energies[:, None] * basis + first_term
    local_projection = jnp.dot(basis.T, image, precision=highest)
    summed_projection, summed_square = lax.psum(
        (local_projection, jnp.dot(image.T, image, precision=highest)), ("row", "col")
    )
    alpha_first = summed_projection / total_rows
    remainder = image - jnp.dot(basis, alpha_first, precision=highest)
    next_gram = summed_square / total_rows - jnp.dot(alpha_first.T, alpha_first, precision=highest)
    lower_next = jnp.linalg.cholesky(next_gram)
    second = jax.scipy.linalg.solve_triangular(lower_next, remainder.T, lower=True).T
    second_term = apply_down(kernel_tile, second.astype(jnp.bfloat16))
    image_next = (
        energies[:, None] * second + second_term - jnp.dot(basis, lower_next, precision=highest)
    )
    alpha_next = (
        lax.psum(jnp.dot(second.T, image_next, precision=highest), ("row", "col")) / total_rows
    )
    residual = image_next - jnp.dot(second, alpha_next, precision=highest)
    return (residual, jnp.stack([alpha_first, lower_next, alpha_next]))


def permute(value, dims, step):
    nz, ny, nx, nc = dims
    pairs = []
    for z in range(nz):
        for y in range(ny):
            for x in range(nx):
                for c in range(nc):
                    source = ((z * ny + y) * nx + x) * nc + c
                    target = (
                        (((z + step[0]) % nz) * ny + (y + step[1]) % ny) * nx + (x + step[2]) % nx
                    ) * nc + (c + step[3]) % nc
                    pairs.append((source, target))
    return lax.ppermute(value, AXES, pairs)


def line_order(nz):
    return [0] + sorted(range(1, nz), key=lambda s: min(s, nz - s))


def gather_everywhere(block, dims, groups, halves=False):
    nz, ny, nx, nc = dims
    line = [block]
    for s in line_order(nz)[1:]:
        line.append(permute(block, dims, (s, 0, 0, 0)))
    found = {}
    for lo, hi in groups:
        own = line[lo] if hi == lo + 1 else jnp.concatenate(line[lo:hi])
        found[(0, 0, 0, lo, hi)] = own
        middle = (lo + hi) // 2
        for y, x in sorted(((y, x) for y in range(ny) for x in range(nx)), key=sum):
            if (y, x) == (0, 0):
                continue
            if halves and y and x and lo < middle:
                at = (middle - lo) * block.shape[0]
                found[(y, x, 0, lo, middle)] = permute(
                    found[(0, x, 0, lo, hi)][:at], dims, (0, y, 0, 0)
                )
                found[(y, x, 0, middle, hi)] = permute(
                    found[(y, 0, 0, lo, hi)][at:], dims, (0, 0, x, 0)
                )
            else:
                found[(y, x, 0, lo, hi)] = permute(own, dims, (0, y, x, 0))
    for y, x, _, lo, hi in list(found):
        for c in range(1, nc):
            found[(y, x, c, lo, hi)] = permute(found[(y, x, 0, lo, hi)], dims, (0, 0, 0, c))
    return list(found.values()), list(found)


def exchange(value, dims, axis, bit):
    nz, ny, nx, nc = dims
    pairs = []
    for z in range(nz):
        for y in range(ny):
            for x in range(nx):
                for c in range(nc):
                    to = [z, y, x, c]
                    to[axis] ^= bit
                    pairs.append(
                        tuple(
                            ((p[0] * ny + p[1]) * nx + p[2]) * nc + p[3]
                            for p in ((z, y, x, c), to)
                        )
                    )
    return lax.ppermute(value, AXES, pairs)


def sum_everywhere(value, dims, order, keep_last=False):
    other = None
    for name in order:
        axis = GRID.index(name)
        n = dims[axis]
        bits = [1 << k for k in range(n.bit_length() - 1)] if n & (n - 1) == 0 else [0]
        for bit in bits:
            if other is not None:
                value = value + other
            if bit:
                other = exchange(value, dims, axis, bit)
            else:
                steps = [[s if k == axis else 0 for k in range(4)] for s in range(1, n)]
                other = sum(permute(value, dims, tuple(step)) for step in steps)
    return (value, other) if keep_last else value + other


def split(value):
    high = value.astype(jnp.bfloat16)
    low = (value - high.astype(jnp.float32)).astype(jnp.bfloat16)
    return high, low


def times(value, weight, transposed):
    high, low = split(value)
    n = value.shape[0]
    both = lax.dot_general(
        jnp.concatenate([high, low]),
        weight,
        (((1,), (1 if transposed else 0,)), ((), ())),
        preferred_element_type=jnp.float32,
    )
    return both[:n] + both[n:]


def nt(a, b):
    return lax.dot_general(
        a, b, (((1,), (1,)), ((), ())), precision=highest, preferred_element_type=jnp.float32
    )


def nn(a, b):
    return lax.dot_general(
        a, b, (((1,), (0,)), ((), ())), precision=highest, preferred_element_type=jnp.float32
    )


def first_kernel(points, neighbor, turned, correlation, payload):
    band = correlation.shape[1]
    columns = turned.shape[0]
    for p in range(points):
        u = times(turned[:, p * band : (p + 1) * band], correlation[p], True)
        payload[pl.ds(p * columns, columns), :] = u.astype(jnp.bfloat16)
    lane = lax.rem(lax.broadcasted_iota(jnp.int32, (16, band), 1), points)
    value = jnp.zeros((16, band), jnp.float32)
    for p in range(points):
        value = jnp.where(lane == p, neighbor[p].astype(jnp.float32), value)
    payload[pl.ds(points * columns, 16), :] = value.astype(jnp.bfloat16)


def wrapped(value, n):
    return lax.rem(value + 2 * n, n)


def place(geometry):
    _, ny, _, nc = geometry.dims
    row, col = lax.axis_index("row"), lax.axis_index("col")
    return row // ny, lax.rem(row, ny), col // nc, lax.rem(col, nc)


def line_step(geometry, line):
    step = jnp.int32(geometry.order[0])
    for k in range(1, len(geometry.order)):
        step = jnp.where(line == k, geometry.order[k], step)
    return step


def weigh_kernel(geometry, pieces, block_rows, with_neighbors, continued, *refs):
    dims, points, columns, band = geometry.dims, geometry.points, geometry.columns, geometry.band
    nz, ny, nx, nc = dims
    n = len(pieces)
    starts = [sum(p[4] - p[3] for p in pieces[:k]) for k in range(n)]
    u_refs, refs = refs[:n], refs[n:]
    weight, refs = refs[0], refs[1:]
    if continued:
        before, refs = refs[:2], refs[2:]
    if with_neighbors:
        acc_0, acc_1, nbs_out, nbv, nbs, sem = refs
        per = band // points
        lane = lax.broadcasted_iota(jnp.int32, (16, band), 1) // points
        rows = [jnp.zeros((16, band), jnp.float32) for _ in range(nbv.shape[0])]
        for index, piece in enumerate(pieces):
            for line in range(piece[4] - piece[3]):
                at = line * block_rows + points * columns
                tile = u_refs[index][pl.ds(at, 16), :].astype(jnp.float32)
                k = starts[index] + line
                rows[k // per] = jnp.where(lane == k % per, tile, rows[k // per])
        for k, row in enumerate(rows):
            nbv[pl.ds(k, 1), :] = row[0:1].astype(jnp.int32)
        copy = pltpu.make_async_copy(nbv, nbs, sem)
        copy.start()
        nbs_out[...] = nbv[...]
    else:
        nbs, acc_0, acc_1 = refs
    sums = (acc_0, acc_1)
    for k in range(2):
        sums[k][...] = before[k][...] if continued else jnp.zeros_like(sums[k])
    if with_neighbors:
        copy.wait()
    z, y, x, c = place(geometry)
    per = band // points
    for index, ref in enumerate(u_refs):
        dy, dx, dc, lo, hi = pieces[index]

        def body(line, carry, ref=ref, index=index, dy=dy, dx=dx, dc=dc, lo=lo):
            device = (
                (wrapped(z - line_step(geometry, line + lo), nz) * ny + wrapped(y - dy, ny)) * nx
                + wrapped(x - dx, nx)
            ) * nc + wrapped(c - dc, nc)
            for q in range(points):
                base = pl.multiple_of(line * block_rows + q * columns, 16)
                u = ref[pl.ds(base, columns), :].astype(jnp.float32)
                k = starts[index] + line
                j = nbs[k // per, lax.rem(k, per) * points + q]
                acc = sums[q % 2]
                for p in range(points):
                    w = weight[p, device * points + q]
                    acc[j, p] += w * u
            return carry

        lax.fori_loop(0, hi - lo, body, 0)


def choose_blocks(geometry, pieces, coarse_refs, own, chosen):
    nz, ny, nx, nc = geometry.dims
    band, per_row, per_col = geometry.band, geometry.per_row, geometry.per_col
    lines = len(geometry.order)
    z, y, x, c = place(geometry)
    for p in range(geometry.points):
        owner_row = own[p] // per_row
        dz = wrapped(z - owner_row // ny, nz)
        dy = wrapped(y - lax.rem(owner_row, ny), ny)
        line = jnp.int32(0)
        for k in range(lines):
            line = jnp.where(dz == geometry.order[k], k, line)
        inner = lax.rem(own[p], per_row)
        for dx in range(nx):
            for dc in range(nc):
                owner_col = wrapped(x - dx, nx) * nc + wrapped(c - dc, nc)
                for k in range(per_col):
                    cut = slice(k * band, (k + 1) * band)
                    block = None
                    for ref, piece in zip(coarse_refs, pieces):
                        if piece[1:3] != (dx, dc):
                            continue
                        lo, hi = piece[3:]
                        at = jnp.clip(line - lo, 0, hi - lo - 1)
                        base = pl.multiple_of((at * per_row + inner) * band, 16)
                        other = ref[pl.ds(base, band), cut]
                        if block is None:
                            block = other
                        else:
                            hit = (dy == piece[0]) & (line >= lo) & (line < hi)
                            block = jnp.where(hit, other, block)
                    chosen[p, owner_col * per_col + k] = block


def image_of(acc_0, acc_1, chosen, correlation, p):
    total = times(acc_0[0, p] + acc_1[0, p], chosen[p, 0], True)
    for j in range(1, acc_0.shape[0]):
        total += times(acc_0[j, p] + acc_1[j, p], chosen[p, j], True)
    return times(total, correlation[p], False)


def first_image_kernel(geometry, pieces, *refs):
    n = len(pieces)
    coarse_refs = refs[:n]
    (acc_0, acc_1, own, correlation, turned, energy, chosen, payload, image) = refs[n:]
    columns, band = geometry.columns, geometry.band
    choose_blocks(geometry, pieces, coarse_refs, own, chosen)
    for p in range(geometry.points):
        cut = slice(p * band, (p + 1) * band)
        value = energy[:, cut] * turned[:, cut] + image_of(acc_0, acc_1, chosen, correlation, p)
        image[:, cut] = value
        payload[pl.ds(p * columns, columns), :] = times(value, correlation[p], True).astype(
            jnp.bfloat16
        )


def gram_kernel(count, turned, image, grams):
    pair = jnp.concatenate([turned[...], image[...]])
    grams[...] = nt(pair, pair) * (1.0 / count)


def second_image_kernel(
    geometry, count, acc_0, acc_1, chosen, correlation, first, energy, image, gram
):
    band = geometry.band
    for p in range(geometry.points):
        cut = slice(p * band, (p + 1) * band)
        image[:, cut] = energy[:, cut] * first[:, cut] + image_of(acc_0, acc_1, chosen, correlation, p)
    gram[...] = nt(first[...], image[...]) * (1.0 / count)


PANEL = 8


def eliminate(work, begin, end):
    n, width = work.shape
    lanes = 128
    rows = lax.broadcasted_iota(jnp.int32, (n, lanes), 0)
    parts = [work[:, k : min(k + lanes, width)] for k in range(0, width, lanes)]
    for at in range(begin, end, PANEL):
        stop = min(at + PANEL, end)
        spread = {
            k: jnp.broadcast_to(parts[k // lanes][:, k % lanes : k % lanes + 1], (n, lanes))
            for k in range(at, stop)
        }
        for k in range(at, stop):
            scale = lax.rsqrt(spread[k][k : k + 1, :])
            column = jnp.where(rows > k, spread[k] * scale, 0.0)
            for j in range(k + 1, stop):
                spread[j] = spread[j] - column * (spread[j][k : k + 1, :] * scale)
            for i, part in enumerate(parts):
                w = part.shape[1]
                pivot = part[k : k + 1, :] * scale[:, :w]
                parts[i] = jnp.where(rows[:, :w] == k, pivot, part - column[:, :w] * pivot)
    return parts[0] if len(parts) == 1 else jnp.concatenate(parts, axis=1)


def unit(m):
    return (
        lax.broadcasted_iota(jnp.int32, (m, m), 0) == lax.broadcasted_iota(jnp.int32, (m, m), 1)
    ).astype(jnp.float32)


def eliminate_kernel_1(joint, out):
    m = joint.shape[0] // 2
    work = jnp.concatenate([joint[:m, :m], unit(m), joint[:m, m:]], axis=1)
    out[...] = eliminate(work, 0, m // 2)


def eliminate_kernel_2(joint, given, out, schur):
    m = joint.shape[0] // 2
    work = eliminate(given[...], m // 2, m)
    out[...] = work
    z1 = work[:, 2 * m :]
    schur[...] = jnp.concatenate([joint[m:, m:] - nn(z1.T, z1), unit(m)], axis=1)


def eliminate_kernel_3(given, out):
    m = given.shape[0]
    out[...] = eliminate(given[...], 0, m // 2)


def eliminate_kernel_4(joint, one, given, turned, first, second, first_two, parts, known, basis):
    m = given.shape[0]
    work = eliminate(given[...], m // 2, m)
    keep = lax.broadcasted_iota(jnp.int32, (m, m), 0) <= lax.broadcasted_iota(jnp.int32, (m, m), 1)
    upper = jnp.where(keep, work[:, :m], 0.0)
    t_x = work[:, m:]
    inverse_first, z1 = one[:, m : 2 * m], one[:, 2 * m :]
    g01, g11 = joint[:m, m:], joint[m:, m:]
    first_two[0] = nt(z1, inverse_first) + SHIFT * unit(m)
    first_two[1] = nn(inverse_first, upper.T)
    t_s = -nn(t_x, nn(z1.T, inverse_first))
    p_s = nn(t_s, g01) + nn(t_x, g11)
    parts[0] = t_x
    parts[1] = nt(p_s, t_s) + nt(nn(t_s, g11), t_x)
    back = nn(nn(upper, inverse_first.T), inverse_first)
    basis[...] = nn(jnp.concatenate([t_s, t_x], axis=1), jnp.concatenate([turned[...], first[...]]))
    known[...] = nn(
        jnp.concatenate([t_s, t_x, -back], axis=1),
        jnp.concatenate([first[...], second[...], turned[...]]),
    )


def last_kernel(gram, other, first_two, parts, known, basis, residual, coefficients):
    g12 = gram[...] + other[...]
    m = g12.shape[0]
    t_x = parts[0]
    alpha_next = parts[1] + nt(nn(t_x, g12), t_x)
    residual[...] = known[...] - nn(alpha_next, basis[...])
    coefficients[0] = first_two[0]
    coefficients[1] = first_two[1]
    coefficients[2] = alpha_next + SHIFT * unit(m)


VMEM = pl.BlockSpec(memory_space=pltpu.VMEM)
SMEM = pl.BlockSpec(memory_space=pltpu.SMEM)


class Geometry:
    def __init__(self, **values):
        self.__dict__.update(values)


def shaped(shape, dtype=jnp.float32):
    return jax.ShapeDtypeStruct(shape, dtype)


def call(kernel, inputs, outputs, scratch=(), work=0.0, aliases=None):
    return pl.pallas_call(
        kernel,
        in_specs=[spec for _, spec in inputs],
        out_shape=outputs,
        out_specs=[VMEM] * len(outputs),
        scratch_shapes=list(scratch),
        input_output_aliases=aliases or {},
        cost_estimate=pl.CostEstimate(
            flops=int(work * FLOPS_PER_US), bytes_accessed=0, transcendentals=0
        ),
        compiler_params=pltpu.CompilerParams(vmem_limit_bytes=48 * 2**20),
    )(*[value for value, _ in inputs])


def weigh(geometry, arrays, pieces, block_rows, weight, neighbors, before=None):
    shape = (geometry.coarse_count, geometry.points, geometry.columns, geometry.band)
    inputs = [(a, VMEM) for a in arrays] + [(weight, SMEM)]
    at = len(inputs)
    if before is not None:
        inputs += [(b, VMEM) for b in before]
    outputs = [shaped(shape), shaped(shape)]
    scratch = []
    blocks = sum(piece[4] - piece[3] for piece in pieces)
    count = pl.cdiv(blocks, geometry.band // geometry.points)
    if neighbors is None:
        outputs.append(shaped((count, geometry.band), jnp.int32))
        scratch = [
            pltpu.VMEM((count, geometry.band), jnp.int32),
            pltpu.SMEM((count, geometry.band), jnp.int32),
            pltpu.SemaphoreType.DMA,
        ]
    else:
        inputs.append((neighbors, SMEM))
    found = call(
        functools.partial(
            weigh_kernel, geometry, pieces, block_rows, neighbors is None, before is not None
        ),
        inputs,
        outputs,
        scratch,
        work=1.0 * len(arrays) / 2,
        aliases={at: 0, at + 1: 1} if before is not None else None,
    )
    return found[:2], found[2:]


def on_device(coarse_kernel, correlations, neighbor, pair_weight, energies, start_block):
    rows, cols = lax.axis_size("row"), lax.axis_size("col")
    points, band, _ = correlations.shape
    columns = start_block.shape[1]
    if rows % 2 or cols % 2 or coarse_kernel.shape[0] % band or coarse_kernel.shape[1] % band or band % points:
        return general_form(
            coarse_kernel, correlations, neighbor, pair_weight, energies, start_block
        )
    dims = (rows // 2, 2, cols // 2, 2)
    order = line_order(dims[0])
    per_row, per_col = coarse_kernel.shape[0] // band, coarse_kernel.shape[1] // band
    geometry = Geometry(
        dims=dims, order=order, points=points, columns=columns, band=band,
        per_row=per_row, per_col=per_col, coarse_count=per_row * rows,
    )
    count = float(start_block.shape[0] * rows * cols)
    half = points * columns
    turned = start_block.T
    own_weight = lax.dynamic_slice_in_dim(
        pair_weight, lax.axis_index("col") * points, points, axis=0
    )
    (payload,) = call(
        functools.partial(first_kernel, points),
        [(neighbor, SMEM), (turned, VMEM), (correlations, VMEM)],
        [shaped((half + 16, band), jnp.bfloat16)],
        work=1.0,
    )
    shifted = energies[None, :] - SHIFT

    nz = dims[0]
    apart = [(0, 1), (1, nz)] if nz > 1 else [(0, 1)]
    u, pieces = gather_everywhere(payload, dims, apart)
    coarse, coarse_pieces = gather_everywhere(coarse_kernel, dims, [(0, nz)], HALVES)

    def group_of(piece):
        y, x, _, lo, _ = piece
        return 0 if lo == 0 or (y, x) == (0, 0) else 1 if y == 0 else 2

    groups = [[k for k, p in enumerate(pieces) if group_of(p) == g] for g in range(3)]
    groups = [group for group in groups if group]
    acc, neighbors = None, []
    for group in groups:
        acc, found = weigh(
            geometry, [u[k] for k in group], [pieces[k] for k in group], half + 16,
            own_weight, None, acc,
        )
        neighbors.append(found[0])
    own = neighbors[0][0, :points]
    coarse_count = geometry.coarse_count
    chosen, payload, first = call(
        functools.partial(first_image_kernel, geometry, coarse_pieces),
        [(a, VMEM) for a in coarse]
        + [(acc[0], VMEM), (acc[1], VMEM), (own, SMEM), (correlations, VMEM), (turned, VMEM), (shifted, VMEM)],
        [
            shaped((points, coarse_count, band, band), jnp.bfloat16),
            shaped((half, band), jnp.bfloat16),
            shaped(turned.shape),
        ],
        work=3.0,
    )
    (joint,) = call(
        functools.partial(gram_kernel, count),
        [(turned, VMEM), (first, VMEM)],
        [shaped((2 * columns, 2 * columns))],
        work=1.0,
    )
    u, _ = gather_everywhere(payload, dims, apart)
    joint = sum_everywhere(joint, dims, "czxy")
    acc = None
    for group, found in zip(groups, neighbors):
        acc, _ = weigh(
            geometry, [u[k] for k in group], [pieces[k] for k in group], half,
            own_weight, found, acc,
        )
    second, g12 = call(
        functools.partial(second_image_kernel, geometry, count),
        [(acc[0], VMEM), (acc[1], VMEM), (chosen, VMEM), (correlations, VMEM), (first, VMEM), (shifted, VMEM)],
        [shaped(turned.shape), shaped((columns, columns))],
        work=3.0,
    )
    m = columns
    (one,) = call(eliminate_kernel_1, [(joint, VMEM)], [shaped((m, 3 * m))], work=3.0)
    one, schur = call(
        eliminate_kernel_2, [(joint, VMEM), (one, VMEM)],
        [shaped((m, 3 * m)), shaped((m, 2 * m))], work=3.0,
    )
    (two,) = call(eliminate_kernel_3, [(schur, VMEM)], [shaped((m, 2 * m))], work=3.0)
    first_two, parts, known, basis = call(
        eliminate_kernel_4,
        [(joint, VMEM), (one, VMEM), (two, VMEM), (turned, VMEM), (first, VMEM), (second, VMEM)],
        [shaped((2, m, m)), shaped((2, m, m)), shaped(turned.shape), shaped(turned.shape)],
        work=3.0,
    )
    g12, other = sum_everywhere(g12, dims, "cxzy", keep_last=True)
    residual, coefficients = call(
        last_kernel,
        [(g12, VMEM), (other, VMEM), (first_two, VMEM), (parts, VMEM), (known, VMEM),
         (basis, VMEM)],
        [shaped(turned.shape), shaped((3, columns, columns))],
        work=2.0,
    )
    return residual.T, coefficients


def solution(mesh):
    in_specs = (
        P("row", "col"),
        P(("row", "col"), None, None),
        P(("row", "col")),
        P("row", None),
        P(("row", "col")),
        P(("row", "col"), None),
    )
    out_specs = (P(("row", "col"), None), P())
    return jax.shard_map(
        on_device, mesh=mesh, in_specs=in_specs, out_specs=out_specs, check_vma=False
    )
```

```python
import functools

import jax
import jax.numpy as jnp
from jax import lax
from jax.experimental import pallas as pl
from jax.experimental.pallas import tpu as pltpu
from jax.sharding import PartitionSpec as P


highest = lax.Precision.HIGHEST
AXES = ("row", "col")
GRID = "zyxc"
SHIFT = 1.25
HALVES = False
FLOPS_PER_US = 5e8


def build_tile(row_correlation, row_neighbor, column_correlation, column_neighbor, coarse, weights):
    band_size = row_correlation.shape[1]
    coarse_count = coarse.shape[0] // band_size
    blocks = coarse.reshape(coarse_count, band_size, coarse_count, band_size)[
        :, :, column_neighbor, :
    ]
    mapped = jnp.einsum(
        "cakb,kbe->cake", blocks, column_correlation, preferred_element_type=jnp.float32
    ).astype(jnp.bfloat16)
    chosen = mapped[row_neighbor]
    product = jnp.einsum(
        "kai,kaje->kije", row_correlation, chosen, preferred_element_type=jnp.float32
    )
    scaled = (product * weights[:, None, :, None]).astype(jnp.bfloat16)
    return scaled.reshape(
        row_correlation.shape[0] * band_size, column_correlation.shape[0] * band_size
    )


def apply_down(kernel_tile, vectors):
    partial_value = jnp.dot(
        kernel_tile,
        lax.all_gather(vectors, "row", axis=0, tiled=True),
        preferred_element_type=jnp.float32,
    )
    return lax.psum_scatter(partial_value, "col", scatter_dimension=0, tiled=True)


def general_form(coarse_kernel, correlations, neighbor, pair_weight, energies, start_block):
    row_correlation, row_neighbor = (
        lax.all_gather(correlations, "col", axis=0, tiled=True),
        lax.all_gather(neighbor, "col", axis=0, tiled=True),
    )
    column_correlation, column_neighbor = (
        lax.all_gather(correlations, "row", axis=0, tiled=True),
        lax.all_gather(neighbor, "row", axis=0, tiled=True),
    )
    coarse_strip = lax.all_gather(coarse_kernel, "row", axis=0, tiled=True)
    coarse = lax.all_gather(coarse_strip, "col", axis=1, tiled=True)
    row_count = lax.axis_size("row")
    col_count = lax.axis_size("col")
    fine_rows = pair_weight.shape[0]
    per_device = fine_rows // col_count
    weight_grid = pair_weight.reshape(fine_rows, row_count, col_count, per_device)
    weights = lax.dynamic_index_in_dim(weight_grid, lax.axis_index("col"), 2, keepdims=False)
    weights = weights.reshape(fine_rows, row_count * per_device)
    kernel_tile = build_tile(
        row_correlation, row_neighbor, column_correlation, column_neighbor, coarse, weights
    )
    total_rows = float(start_block.shape[0] * row_count * col_count)
    first_gram = (
        lax.psum(jnp.dot(start_block.T, start_block, precision=highest), ("row", "col"))
        / total_rows
    )
    lower_first = jnp.linalg.cholesky(first_gram)
    basis = jax.scipy.linalg.solve_triangular(lower_first, start_block.T, lower=True).T
    first_term = apply_down(kernel_tile, basis.astype(jnp.bfloat16))
    image = energies[:, None] * basis + first_term
    local_projection = jnp.dot(basis.T, image, precision=highest)
    summed_projection, summed_square = lax.psum(
        (local_projection, jnp.dot(image.T, image, precision=highest)), ("row", "col")
    )
    alpha_first = summed_projection / total_rows
    remainder = image - jnp.dot(basis, alpha_first, precision=highest)
    next_gram = summed_square / total_rows - jnp.dot(alpha_first.T, alpha_first, precision=highest)
    lower_next = jnp.linalg.cholesky(next_gram)
    second = jax.scipy.linalg.solve_triangular(lower_next, remainder.T, lower=True).T
    second_term = apply_down(kernel_tile, second.astype(jnp.bfloat16))
    image_next = (
        energies[:, None] * second + second_term - jnp.dot(basis, lower_next, precision=highest)
    )
    alpha_next = (
        lax.psum(jnp.dot(second.T, image_next, precision=highest), ("row", "col")) / total_rows
    )
    residual = image_next - jnp.dot(second, alpha_next, precision=highest)
    return (residual, jnp.stack([alpha_first, lower_next, alpha_next]))


def permute(value, dims, step):
    nz, ny, nx, nc = dims
    pairs = []
    for z in range(nz):
        for y in range(ny):
            for x in range(nx):
                for c in range(nc):
                    source = ((z * ny + y) * nx + x) * nc + c
                    target = (
                        (((z + step[0]) % nz) * ny + (y + step[1]) % ny) * nx + (x + step[2]) % nx
                    ) * nc + (c + step[3]) % nc
                    pairs.append((source, target))
    return lax.ppermute(value, AXES, pairs)


def line_order(nz):
    return [0] + sorted(range(1, nz), key=lambda s: min(s, nz - s))


def gather_everywhere(block, dims, groups, halves=False):
    nz, ny, nx, nc = dims
    line = [block]
    for s in line_order(nz)[1:]:
        line.append(permute(block, dims, (s, 0, 0, 0)))
    found = {}
    for lo, hi in groups:
        own = line[lo] if hi == lo + 1 else jnp.concatenate(line[lo:hi])
        found[(0, 0, 0, lo, hi)] = own
        middle = (lo + hi) // 2
        for y, x in sorted(((y, x) for y in range(ny) for x in range(nx)), key=sum):
            if (y, x) == (0, 0):
                continue
            if halves and y and x and lo < middle:
                at = (middle - lo) * block.shape[0]
                found[(y, x, 0, lo, middle)] = permute(
                    found[(0, x, 0, lo, hi)][:at], dims, (0, y, 0, 0)
                )
                found[(y, x, 0, middle, hi)] = permute(
                    found[(y, 0, 0, lo, hi)][at:], dims, (0, 0, x, 0)
                )
            else:
                found[(y, x, 0, lo, hi)] = permute(own, dims, (0, y, x, 0))
    for y, x, _, lo, hi in list(found):
        for c in range(1, nc):
            found[(y, x, c, lo, hi)] = permute(found[(y, x, 0, lo, hi)], dims, (0, 0, 0, c))
    return list(found.values()), list(found)


def exchange(value, dims, axis, bit):
    nz, ny, nx, nc = dims
    pairs = []
    for z in range(nz):
        for y in range(ny):
            for x in range(nx):
                for c in range(nc):
                    to = [z, y, x, c]
                    to[axis] ^= bit
                    pairs.append(
                        tuple(
                            ((p[0] * ny + p[1]) * nx + p[2]) * nc + p[3]
                            for p in ((z, y, x, c), to)
                        )
                    )
    return lax.ppermute(value, AXES, pairs)


def sum_everywhere(value, dims, order, keep_last=False):
    other = None
    for name in order:
        axis = GRID.index(name)
        n = dims[axis]
        bits = [1 << k for k in range(n.bit_length() - 1)] if n & (n - 1) == 0 else [0]
        for bit in bits:
            if other is not None:
                value = value + other
            if bit:
                other = exchange(value, dims, axis, bit)
            else:
                steps = [[s if k == axis else 0 for k in range(4)] for s in range(1, n)]
                other = sum(permute(value, dims, tuple(step)) for step in steps)
    return (value, other) if keep_last else value + other


def split(value):
    high = value.astype(jnp.bfloat16)
    low = (value - high.astype(jnp.float32)).astype(jnp.bfloat16)
    return high, low


def times(value, weight, transposed):
    high, low = split(value)
    n = value.shape[0]
    both = lax.dot_general(
        jnp.concatenate([high, low]),
        weight,
        (((1,), (1 if transposed else 0,)), ((), ())),
        preferred_element_type=jnp.float32,
    )
    return both[:n] + both[n:]


def nt(a, b):
    return lax.dot_general(
        a, b, (((1,), (1,)), ((), ())), precision=highest, preferred_element_type=jnp.float32
    )


def nn(a, b):
    return lax.dot_general(
        a, b, (((1,), (0,)), ((), ())), precision=highest, preferred_element_type=jnp.float32
    )


def first_kernel(points, neighbor, turned, correlation, payload):
    band = correlation.shape[1]
    columns = turned.shape[0]
    for p in range(points):
        u = times(turned[:, p * band : (p + 1) * band], correlation[p], True)
        payload[pl.ds(p * columns, columns), :] = u.astype(jnp.bfloat16)
    lane = lax.rem(lax.broadcasted_iota(jnp.int32, (16, band), 1), points)
    value = jnp.zeros((16, band), jnp.float32)
    for p in range(points):
        value = jnp.where(lane == p, neighbor[p].astype(jnp.float32), value)
    payload[pl.ds(points * columns, 16), :] = value.astype(jnp.bfloat16)


def wrapped(value, n):
    return lax.rem(value + 2 * n, n)


def place(geometry):
    _, ny, _, nc = geometry.dims
    row, col = lax.axis_index("row"), lax.axis_index("col")
    return row // ny, lax.rem(row, ny), col // nc, lax.rem(col, nc)


def line_step(geometry, line):
    step = jnp.int32(geometry.order[0])
    for k in range(1, len(geometry.order)):
        step = jnp.where(line == k, geometry.order[k], step)
    return step


def weigh_kernel(geometry, pieces, block_rows, with_neighbors, continued, *refs):
    dims, points, columns, band = geometry.dims, geometry.points, geometry.columns, geometry.band
    nz, ny, nx, nc = dims
    n = len(pieces)
    starts = [sum(p[4] - p[3] for p in pieces[:k]) for k in range(n)]
    u_refs, refs = refs[:n], refs[n:]
    weight, refs = refs[0], refs[1:]
    if continued:
        before, refs = refs[:2], refs[2:]
    if with_neighbors:
        acc_0, acc_1, nbs_out, nbv, nbs, sem = refs
        per = band // points
        lane = lax.broadcasted_iota(jnp.int32, (16, band), 1) // points
        rows = [jnp.zeros((16, band), jnp.float32) for _ in range(nbv.shape[0])]
        for index, piece in enumerate(pieces):
            for line in range(piece[4] - piece[3]):
                at = line * block_rows + points * columns
                tile = u_refs[index][pl.ds(at, 16), :].astype(jnp.float32)
                k = starts[index] + line
                rows[k // per] = jnp.where(lane == k % per, tile, rows[k // per])
        for k, row in enumerate(rows):
            nbv[pl.ds(k, 1), :] = row[0:1].astype(jnp.int32)
        copy = pltpu.make_async_copy(nbv, nbs, sem)
        copy.start()
        nbs_out[...] = nbv[...]
    else:
        nbs, acc_0, acc_1 = refs
    sums = (acc_0, acc_1)
    for k in range(2):
        sums[k][...] = before[k][...] if continued else jnp.zeros_like(sums[k])
    if with_neighbors:
        copy.wait()
    z, y, x, c = place(geometry)
    per = band // points
    for index, ref in enumerate(u_refs):
        dy, dx, dc, lo, hi = pieces[index]

        def body(line, carry, ref=ref, index=index, dy=dy, dx=dx, dc=dc, lo=lo):
            device = (
                (wrapped(z - line_step(geometry, line + lo), nz) * ny + wrapped(y - dy, ny)) * nx
                + wrapped(x - dx, nx)
            ) * nc + wrapped(c - dc, nc)
            for q in range(points):
                base = pl.multiple_of(line * block_rows + q * columns, 16)
                u = ref[pl.ds(base, columns), :].astype(jnp.float32)
                k = starts[index] + line
                j = nbs[k // per, lax.rem(k, per) * points + q]
                acc = sums[q % 2]
                for p in range(points):
                    w = weight[p, device * points + q]
                    acc[j, p] += w * u
            return carry

        lax.fori_loop(0, hi - lo, body, 0)


def choose_blocks(geometry, pieces, coarse_refs, own, chosen):
    nz, ny, nx, nc = geometry.dims
    band, per_row, per_col = geometry.band, geometry.per_row, geometry.per_col
    lines = len(geometry.order)
    z, y, x, c = place(geometry)
    for p in range(geometry.points):
        owner_row = own[p] // per_row
        dz = wrapped(z - owner_row // ny, nz)
        dy = wrapped(y - lax.rem(owner_row, ny), ny)
        line = jnp.int32(0)
        for k in range(lines):
            line = jnp.where(dz == geometry.order[k], k, line)
        inner = lax.rem(own[p], per_row)
        for dx in range(nx):
            for dc in range(nc):
                owner_col = wrapped(x - dx, nx) * nc + wrapped(c - dc, nc)
                for k in range(per_col):
                    cut = slice(k * band, (k + 1) * band)
                    block = None
                    for ref, piece in zip(coarse_refs, pieces):
                        if piece[1:3] != (dx, dc):
                            continue
                        lo, hi = piece[3:]
                        at = jnp.clip(line - lo, 0, hi - lo - 1)
                        base = pl.multiple_of((at * per_row + inner) * band, 16)
                        other = ref[pl.ds(base, band), cut]
                        if block is None:
                            block = other
                        else:
                            hit = (dy == piece[0]) & (line >= lo) & (line < hi)
                            block = jnp.where(hit, other, block)
                    chosen[p, owner_col, :, k * band : (k + 1) * band] = block


def image_of(acc_0, acc_1, chosen, correlation, p):
    total = None
    groups = chosen.shape[1]
    per_col = acc_0.shape[0] // groups
    for g in range(groups):
        sums = [
            (acc_0[j, p] + acc_1[j, p]).astype(jnp.bfloat16)
            for j in range(g * per_col, (g + 1) * per_col)
        ]
        part = lax.dot_general(
            sums[0] if per_col == 1 else jnp.concatenate(sums, axis=1),
            chosen[p, g],
            (((1,), (1,)), ((), ())),
            preferred_element_type=jnp.float32,
        )
        total = part if total is None else total + part
    return times(total, correlation[p], False)


def first_image_kernel(geometry, pieces, *refs):
    n = len(pieces)
    coarse_refs = refs[:n]
    (acc_0, acc_1, own, correlation, turned, energy, chosen, payload, image) = refs[n:]
    columns, band = geometry.columns, geometry.band
    choose_blocks(geometry, pieces, coarse_refs, own, chosen)
    for p in range(geometry.points):
        cut = slice(p * band, (p + 1) * band)
        value = energy[:, cut] * turned[:, cut] + image_of(acc_0, acc_1, chosen, correlation, p)
        image[:, cut] = value
        payload[pl.ds(p * columns, columns), :] = times(value, correlation[p], True).astype(
            jnp.bfloat16
        )


def gram_kernel(count, turned, image, grams):
    pair = jnp.concatenate([turned[...], image[...]])
    grams[...] = nt(pair, pair) * (1.0 / count)


def second_image_kernel(
    geometry, count, acc_0, acc_1, chosen, correlation, first, energy, image, gram
):
    band = geometry.band
    for p in range(geometry.points):
        cut = slice(p * band, (p + 1) * band)
        image[:, cut] = energy[:, cut] * first[:, cut] + image_of(acc_0, acc_1, chosen, correlation, p)
    gram[...] = nt(first[...], image[...]) * (1.0 / count)


PANEL = 8


def eliminate(work, begin, end):
    n, width = work.shape
    lanes = 128
    rows = lax.broadcasted_iota(jnp.int32, (n, lanes), 0)
    parts = [work[:, k : min(k + lanes, width)] for k in range(0, width, lanes)]
    for at in range(begin, end, PANEL):
        stop = min(at + PANEL, end)
        spread = {
            k: jnp.broadcast_to(parts[k // lanes][:, k % lanes : k % lanes + 1], (n, lanes))
            for k in range(at, stop)
        }
        for k in range(at, stop):
            scale = lax.rsqrt(spread[k][k : k + 1, :])
            column = jnp.where(rows > k, spread[k] * scale, 0.0)
            for j in range(k + 1, stop):
                spread[j] = spread[j] - column * (spread[j][k : k + 1, :] * scale)
            for i, part in enumerate(parts):
                w = part.shape[1]
                pivot = part[k : k + 1, :] * scale[:, :w]
                parts[i] = jnp.where(rows[:, :w] == k, pivot, part - column[:, :w] * pivot)
    return parts[0] if len(parts) == 1 else jnp.concatenate(parts, axis=1)


def unit(m):
    return (
        lax.broadcasted_iota(jnp.int32, (m, m), 0) == lax.broadcasted_iota(jnp.int32, (m, m), 1)
    ).astype(jnp.float32)


def eliminate_kernel_1(joint, out):
    m = joint.shape[0] // 2
    work = jnp.concatenate([joint[:m, :m], unit(m), joint[:m, m:]], axis=1)
    out[...] = eliminate(work, 0, m // 2)


def eliminate_kernel_2(joint, given, out, schur):
    m = joint.shape[0] // 2
    work = eliminate(given[...], m // 2, m)
    out[...] = work
    z1 = work[:, 2 * m :]
    schur[...] = jnp.concatenate([joint[m:, m:] - nn(z1.T, z1), unit(m)], axis=1)


def eliminate_kernel_3(given, out):
    m = given.shape[0]
    out[...] = eliminate(given[...], 0, m // 2)


def eliminate_kernel_4(joint, one, given, turned, first, second, first_two, parts, known, basis):
    m = given.shape[0]
    work = eliminate(given[...], m // 2, m)
    keep = lax.broadcasted_iota(jnp.int32, (m, m), 0) <= lax.broadcasted_iota(jnp.int32, (m, m), 1)
    upper = jnp.where(keep, work[:, :m], 0.0)
    t_x = work[:, m:]
    inverse_first, z1 = one[:, m : 2 * m], one[:, 2 * m :]
    g01, g11 = joint[:m, m:], joint[m:, m:]
    first_two[0] = nt(z1, inverse_first) + SHIFT * unit(m)
    first_two[1] = nn(inverse_first, upper.T)
    t_s = -nn(t_x, nn(z1.T, inverse_first))
    p_s = nn(t_s, g01) + nn(t_x, g11)
    back = nn(nn(upper, inverse_first.T), inverse_first)
    across = nn(t_s, joint[:m, :m]) + nn(t_x, joint[m:, :m])
    parts[0] = t_x
    parts[1] = nt(p_s, t_s) + nt(nn(t_s, g11), t_x) - nt(across, back)
    basis[...] = nn(jnp.concatenate([t_s, t_x], axis=1), jnp.concatenate([turned[...], first[...]]))
    known[...] = nn(
        jnp.concatenate([t_s, t_x, -back], axis=1),
        jnp.concatenate([first[...], second[...], turned[...]]),
    )


def last_kernel(gram, other, first_two, parts, known, basis, residual, coefficients):
    g12 = gram[...] + other[...]
    m = g12.shape[0]
    t_x = parts[0]
    alpha_next = parts[1] + nt(nn(t_x, g12), t_x)
    residual[...] = known[...] - nn(alpha_next, basis[...])
    coefficients[0] = first_two[0]
    coefficients[1] = first_two[1]
    coefficients[2] = alpha_next + SHIFT * unit(m)


VMEM = pl.BlockSpec(memory_space=pltpu.VMEM)
SMEM = pl.BlockSpec(memory_space=pltpu.SMEM)


class Geometry:
    def __init__(self, **values):
        self.__dict__.update(values)


def shaped(shape, dtype=jnp.float32):
    return jax.ShapeDtypeStruct(shape, dtype)


def call(kernel, inputs, outputs, scratch=(), work=0.0, aliases=None):
    return pl.pallas_call(
        kernel,
        in_specs=[spec for _, spec in inputs],
        out_shape=outputs,
        out_specs=[VMEM] * len(outputs),
        scratch_shapes=list(scratch),
        input_output_aliases=aliases or {},
        cost_estimate=pl.CostEstimate(
            flops=int(work * FLOPS_PER_US), bytes_accessed=0, transcendentals=0
        ),
        compiler_params=pltpu.CompilerParams(vmem_limit_bytes=48 * 2**20),
    )(*[value for value, _ in inputs])


def weigh(geometry, arrays, pieces, block_rows, weight, neighbors, before=None):
    shape = (geometry.coarse_count, geometry.points, geometry.columns, geometry.band)
    inputs = [(a, VMEM) for a in arrays] + [(weight, SMEM)]
    at = len(inputs)
    if before is not None:
        inputs += [(b, VMEM) for b in before]
    outputs = [shaped(shape), shaped(shape)]
    scratch = []
    blocks = sum(piece[4] - piece[3] for piece in pieces)
    count = pl.cdiv(blocks, geometry.band // geometry.points)
    if neighbors is None:
        outputs.append(shaped((count, geometry.band), jnp.int32))
        scratch = [
            pltpu.VMEM((count, geometry.band), jnp.int32),
            pltpu.SMEM((count, geometry.band), jnp.int32),
            pltpu.SemaphoreType.DMA,
        ]
    else:
        inputs.append((neighbors, SMEM))
    found = call(
        functools.partial(
            weigh_kernel, geometry, pieces, block_rows, neighbors is None, before is not None
        ),
        inputs,
        outputs,
        scratch,
        work=1.0 * len(arrays) / 2,
        aliases={at: 0, at + 1: 1} if before is not None else None,
    )
    return found[:2], found[2:]


def on_device(coarse_kernel, correlations, neighbor, pair_weight, energies, start_block):
    rows, cols = lax.axis_size("row"), lax.axis_size("col")
    points, band, _ = correlations.shape
    columns = start_block.shape[1]
    if rows % 2 or cols % 2 or coarse_kernel.shape[0] % band or coarse_kernel.shape[1] % band or band % points:
        return general_form(
            coarse_kernel, correlations, neighbor, pair_weight, energies, start_block
        )
    dims = (rows // 2, 2, cols // 2, 2)
    order = line_order(dims[0])
    per_row, per_col = coarse_kernel.shape[0] // band, coarse_kernel.shape[1] // band
    geometry = Geometry(
        dims=dims, order=order, points=points, columns=columns, band=band,
        per_row=per_row, per_col=per_col, coarse_count=per_row * rows,
    )
    count = float(start_block.shape[0] * rows * cols)
    half = points * columns
    turned = start_block.T
    own_weight = lax.dynamic_slice_in_dim(
        pair_weight, lax.axis_index("col") * points, points, axis=0
    )
    (payload,) = call(
        functools.partial(first_kernel, points),
        [(neighbor, SMEM), (turned, VMEM), (correlations, VMEM)],
        [shaped((half + 16, band), jnp.bfloat16)],
        work=1.0,
    )
    shifted = energies[None, :] - SHIFT

    nz = dims[0]
    apart = [(0, 1), (1, nz)] if nz > 1 else [(0, 1)]
    u, pieces = gather_everywhere(payload, dims, apart)
    coarse, coarse_pieces = gather_everywhere(coarse_kernel, dims, [(0, nz)], HALVES)

    def group_of(piece):
        y, x, _, lo, _ = piece
        return 0 if lo == 0 or (y, x) == (0, 0) else 1 if y == 0 else 2

    groups = [[k for k, p in enumerate(pieces) if group_of(p) == g] for g in range(3)]
    groups = [group for group in groups if group]
    acc, neighbors = None, []
    for group in groups:
        acc, found = weigh(
            geometry, [u[k] for k in group], [pieces[k] for k in group], half + 16,
            own_weight, None, acc,
        )
        neighbors.append(found[0])
    own = neighbors[0][0, :points]
    chosen, payload, first = call(
        functools.partial(first_image_kernel, geometry, coarse_pieces),
        [(a, VMEM) for a in coarse]
        + [(acc[0], VMEM), (acc[1], VMEM), (own, SMEM), (correlations, VMEM), (turned, VMEM), (shifted, VMEM)],
        [
            shaped((points, cols, band, per_col * band), jnp.bfloat16),
            shaped((half, band), jnp.bfloat16),
            shaped(turned.shape),
        ],
        work=3.0,
    )
    (joint,) = call(
        functools.partial(gram_kernel, count),
        [(turned, VMEM), (first, VMEM)],
        [shaped((2 * columns, 2 * columns))],
        work=1.0,
    )
    u, _ = gather_everywhere(payload, dims, apart)
    joint = sum_everywhere(joint, dims, "czxy")
    acc = None
    for group, found in zip(groups, neighbors):
        acc, _ = weigh(
            geometry, [u[k] for k in group], [pieces[k] for k in group], half,
            own_weight, found, acc,
        )
    second, g12 = call(
        functools.partial(second_image_kernel, geometry, count),
        [(acc[0], VMEM), (acc[1], VMEM), (chosen, VMEM), (correlations, VMEM), (first, VMEM), (shifted, VMEM)],
        [shaped(turned.shape), shaped((columns, columns))],
        work=3.0,
    )
    m = columns
    (one,) = call(eliminate_kernel_1, [(joint, VMEM)], [shaped((m, 3 * m))], work=3.0)
    one, schur = call(
        eliminate_kernel_2, [(joint, VMEM), (one, VMEM)],
        [shaped((m, 3 * m)), shaped((m, 2 * m))], work=3.0,
    )
    (two,) = call(eliminate_kernel_3, [(schur, VMEM)], [shaped((m, 2 * m))], work=3.0)
    first_two, parts, known, basis = call(
        eliminate_kernel_4,
        [(joint, VMEM), (one, VMEM), (two, VMEM), (turned, VMEM), (first, VMEM), (second, VMEM)],
        [shaped((2, m, m)), shaped((2, m, m)), shaped(turned.shape), shaped(turned.shape)],
        work=3.0,
    )
    g12, other = sum_everywhere(g12, dims, "cxzy", keep_last=True)
    residual, coefficients = call(
        last_kernel,
        [(g12, VMEM), (other, VMEM), (first_two, VMEM), (parts, VMEM), (known, VMEM),
         (basis, VMEM)],
        [shaped(turned.shape), shaped((3, columns, columns))],
        work=2.0,
    )
    return residual.T, coefficients


def solution(mesh):
    in_specs = (
        P("row", "col"),
        P(("row", "col"), None, None),
        P(("row", "col")),
        P("row", None),
        P(("row", "col")),
        P(("row", "col"), None),
    )
    out_specs = (P(("row", "col"), None), P())
    return jax.shard_map(
        on_device, mesh=mesh, in_specs=in_specs, out_specs=out_specs, check_vma=False
    )
```
